32 devices in a mesh: frame: 8 (over z, y), head: 4 (over x, core).
Axes of the slice: x: 2, y: 2, z: 4, core: 2. Of those that a mesh axis runs over, the one named last changes fastest.
Arguments:
- latents: bfloat16 [4096, 5120], P('frame', 'head'), may hold values from -6 to 6
- queries: bfloat16 [4096, 2560], P('frame', 'head'), may hold values from -22 to 22
- keys: bfloat16 [4096, 2560], P('frame', 'head'), may hold values from -6 to 6
- values: bfloat16 [4096, 2560], P('frame', 'head'), may hold values from -6 to 6
- out_weight: bfloat16 [2560, 5120], P('head'), may hold values from -0.5 to 0.5
- gate_table: float32 [4, 5120], P(None, 'head'), may hold values from 0.5 to 2
- levels: int32 [8], P('frame'), may hold values from 0 to 3
- block_mask: int32 [8, 4], P('frame'), may hold values from 0 to 1, as said below
- fresh: bfloat16 [512, 5120], P(None, 'head'), may hold values from -6 to 6
Outputs:
- velocity: bfloat16 [4096, 5120], P('frame', 'head')
- next_latents: bfloat16 [4096, 5120], P('frame', 'head')
The draws below stay inside these ranges and needn't reach their ends.
Inputs may be any that keep to these rules, and one draw needn't show every extreme that they name: block_mask[c, 0] is 1 for every span c.
All inputs are finite; a program needn't handle non-finite values.
Results may differ from the reference program's by a relative error of at most 0.012.
Values may be sent and summed in bfloat16 or wider, within the bound.
A program may use at most 128 MiB of HBM per device.

```python
import math
import jax
import jax.numpy as jnp
from jax import lax

D = 5120
HEADS = 20
HD = 128
WIN = 4
LEVELS = 4
TOK_DEV = 512
SPANS = 8
TOKENS = 4096
HH = 2560
N_HEAD = 4


def draw_pair(key):
    key_query, key_key = jax.random.split(key, 2)
    query_draw = jnp.clip(jax.random.normal(key_query, (TOKENS, HH), jnp.float32) * 2.0, -12.0, 12.0)
    key_draw = jax.random.normal(key_key, (TOKENS, HH), jnp.float32)
    query_draw = jnp.clip(query_draw, -22.0, 22.0)
    key_draw = jnp.clip(key_draw, -6.0, 6.0)
    return (query_draw, key_draw)


def draw_queries(key, part):
    pair = draw_pair(jax.random.fold_in(key, 17))
    return pair[0].astype(jnp.bfloat16)


def draw_keys(key, part):
    pair = draw_pair(jax.random.fold_in(key, 17))
    return pair[1].astype(jnp.bfloat16)


def draw_block_mask(key, part):
    picks = jax.random.randint(jax.random.fold_in(key, 29), (SPANS, WIN), 0, 10)
    marks = (picks < 7).astype(jnp.int32)
    column = jnp.arange(WIN)[None, :]
    return jnp.where(column == 0, 1, marks).astype(jnp.int32)


def with_ends(entries, rng, smallest, high):
    dims = entries.shape
    index_at = [jax.random.randint(jax.random.fold_in(rng, axis), (), 0, dims[axis]) for axis in range(len(dims))]
    entries = entries.at[tuple(index_at)].set(smallest)
    longest = dims.index(max(dims))
    index_at[longest] = (index_at[longest] + 1) % dims[longest]
    return entries.at[tuple(index_at)].set(high)


def shard_levels(rng, extent, shards, smallest, high):
    level, own = 1.0, jax.random.fold_in(rng, 6)
    for axis_at, parts in shards:
        heights = jnp.exp(jax.random.uniform(jax.random.fold_in(own, axis_at), (parts,), jnp.float32, smallest / len(shards), high / len(shards)))
        level = level * jnp.repeat(heights, extent[axis_at] // parts).reshape([-1 if axis == axis_at else 1 for axis in range(len(extent))])
    return level


def centred(own_key, extent, deviation, reach, cuts=(), kind=jnp.bfloat16):
    entries = deviation * jax.random.normal(own_key, extent, jnp.float32)
    if cuts:
        entries = entries * shard_levels(own_key, extent, cuts, -0.22, 0.18)
    return jnp.clip(entries, -reach, reach).astype(kind)


def setup_inputs(seed: int = 0) -> dict:
    seeds = jax.random.split(jax.random.key(seed), 10)
    latents = centred(seeds[0], (TOKENS, D), 1.0, 6.0, ((0, 8), (1, 4)))
    queries = draw_queries(jax.random.fold_in(seeds[9], 71), 0)
    keys = draw_keys(jax.random.fold_in(seeds[9], 71), 0)
    values = centred(seeds[3], (TOKENS, HH), 1.0, 6.0, ((0, 8), (1, 4)))
    out_weight = centred(seeds[4], (HH, D), HD ** -0.5, 0.5, ((0, 4),))
    gate_table = jnp.clip(0.5 + 1.5 * jax.random.uniform(seeds[5], (LEVELS, D), jnp.float32) ** shard_levels(seeds[5], (LEVELS, D), ((1, 4),), -0.2, 0.2), 0.5, 2.0)
    levels = with_ends(jax.random.randint(seeds[6], (SPANS,), 0, LEVELS), jax.random.fold_in(seeds[6], 1), 0, LEVELS - 1).astype(jnp.int32)
    block_mask = draw_block_mask(jax.random.fold_in(seeds[9], 71), 0)
    fresh = centred(seeds[8], (TOK_DEV, D), 1.0, 6.0, ((1, 4),))
    return dict(latents=latents, queries=queries, keys=keys, values=values, out_weight=out_weight, gate_table=gate_table, levels=levels, block_mask=block_mask, fresh=fresh)


flow_shift = 5.0

def noise_level(point):
    return flow_shift * point / (1.0 + (flow_shift - 1.0) * point)

def reference(latents, queries, keys, values, out_weight, gate_table, levels, block_mask, fresh):
    group = HH // N_HEAD
    scale = 1.0 / math.sqrt(HD)
    padding = jnp.zeros(((WIN - 1) * TOK_DEV, HH), keys.dtype)
    key_padded = jnp.concatenate([padding, keys], 0)
    value_padded = jnp.concatenate([padding, values], 0)

    def one_span(span):
        start = (span * TOK_DEV).astype(jnp.int32)
        query_rows = lax.dynamic_slice_in_dim(queries, start, TOK_DEV, 0).astype(jnp.float32).reshape(TOK_DEV, HEADS, HD)
        key_rows = lax.dynamic_slice_in_dim(key_padded, start, WIN * TOK_DEV, 0).reshape(WIN, TOK_DEV, HEADS, HD)
        key_rows = jnp.flip(key_rows, 0).astype(jnp.float32)
        value_rows = lax.dynamic_slice_in_dim(value_padded, start, WIN * TOK_DEV, 0).reshape(WIN, TOK_DEV, HEADS, HD)
        value_rows = jnp.flip(value_rows, 0).astype(jnp.float32)
        distances = jnp.arange(WIN, dtype=jnp.int32)
        allowed = (block_mask[span] == 1) & (span - distances >= 0)
        scores = jnp.einsum('qhd,bkhd->hqbk', query_rows, key_rows) * scale
        scores = jnp.where(allowed[None, None, :, None], scores, -jnp.inf)
        top = lax.optimization_barrier(jnp.max(scores, axis=(2, 3), keepdims=True))
        expd = jnp.exp(scores - top)
        weights = (expd / lax.optimization_barrier(jnp.sum(expd, axis=(2, 3), keepdims=True))).astype(jnp.bfloat16)
        attended = jnp.einsum('hqbk,bkhd->qhd', weights.astype(jnp.float32), value_rows)
        attended = attended.reshape(TOK_DEV, HH).astype(jnp.bfloat16)
        total = jnp.zeros((TOK_DEV, D), jnp.float32)
        for index in range(N_HEAD):
            part = jnp.dot(attended[:, index * group:(index + 1) * group], out_weight[index * group:(index + 1) * group], preferred_element_type=jnp.float32)
            rounded = lax.optimization_barrier(part.astype(jnp.bfloat16))
            total = total + rounded.astype(jnp.float32)
        return total
    projected = lax.map(one_span, jnp.arange(SPANS, dtype=jnp.int32))
    level_float = levels.astype(jnp.float32)
    delta = noise_level(level_float / LEVELS) - noise_level((level_float + 1.0) / LEVELS)
    gate = gate_table[levels]
    gated = gate[:, None, :] * projected
    velocity = gated.astype(jnp.bfloat16).reshape(TOKENS, D)
    updated = latents.reshape(SPANS, TOK_DEV, D).astype(jnp.float32) + delta[:, None, None] * gated
    moved = updated[1:].reshape((SPANS - 1) * TOK_DEV, D).astype(jnp.bfloat16)
    next_latents = jnp.concatenate([moved, fresh], 0)
    return (velocity, next_latents)
```

```python
import functools
import math

import jax
import jax.numpy as jnp
from jax import lax
from jax.experimental import pallas as pl
from jax.experimental.pallas import tpu as pltpu
from jax.sharding import PartitionSpec as P

HD = 128
LANES = 128
LEVELS = 4
FAR = 1e30
LOW = -1e20

flow_shift = 5.0

MESH = pl.DeviceIdType.MESH
bf16 = jnp.bfloat16
f32 = jnp.float32


def noise_level(point):
    return flow_shift * point / (1.0 + (flow_shift - 1.0) * point)


def partial_attention(query, blocks, penalties):
    scale = math.log2(math.e) / math.sqrt(HD)
    scores = [
        lax.dot_general(query, k, (((1,), (1,)), ((), ())), preferred_element_type=f32) * scale
        for k, _ in blocks
    ]
    top = LOW
    for s, penalty in zip(scores, penalties):
        top = jnp.maximum(top, jnp.max(s, axis=1, keepdims=True) - penalty)
    acc = 0.0
    for s, penalty, (_, v) in zip(scores, penalties, blocks):
        weights = jnp.exp2(s - (top + penalty)).astype(bf16)
        wide = jnp.concatenate([v, jnp.ones((v.shape[0], LANES), bf16)], axis=1)
        acc = acc + jnp.dot(weights, wide, preferred_element_type=f32)
    total = jnp.maximum(acc[:, HD:], 1.0)
    return acc[:, :HD] / total, top + jnp.log2(total)


def kernel(
    levels_ref, mask_ref, q_hbm, k_hbm, v_hbm, w_hbm, lat_hbm, fresh_hbm, gate_ref,
    vel_hbm, next_hbm,
    q_own, k_own, v_own, q_guest, k_prev, v_prev, pen_own, pen_guest,
    o_send, o_recv, st_send, st_recv, o_loc, lse_loc, attended, w_ref, lat_ref, gate_row,
    pair_send, pair_recv, near_send, near_recv, far_send, far_recv, vel_stage, upd_stage,
    in_sem, bulk_sem, kv_ss, kv_rs, q_ss, q_rs, o_ss, o_rs, st_ss, st_rs, pen_sem,
    pair_ss, pair_rs, near_ss, near_rs, far_ss, far_rs, vel_sem, slide_ss, slide_rs,
):
    f = lax.axis_index("frame")
    frames = lax.axis_size("frame")
    me = lax.axis_index("head")
    heads, span, _ = q_own.shape
    pieces, prow, pcol = pair_send.shape
    row_parts = span // prow
    out_width = lat_ref.shape[1]
    tile = min(span, 256)

    pair = me + 1 - 2 * (me % 2)
    far = (me + 2) % 4
    has_prev = f >= 1
    has_down = f >= 2
    has_next = f + 1 < frames
    has_up = f + 2 < frames

    def remote(src, dst, ss, rs, frame=None, head=None):
        where = {"frame": frame} if head is None else {"head": head}
        return pltpu.make_async_remote_copy(
            src_ref=src, dst_ref=dst, send_sem=ss, recv_sem=rs, device_id=where, device_id_type=MESH
        )

    def columns(h):
        return pl.ds(pl.multiple_of(h * HD, HD), HD)

    def local_in(h):
        return [
            pltpu.make_async_copy(src.at[:, columns(h)], dst.at[h], in_sem.at[h, i])
            for i, (src, dst) in enumerate(((k_hbm, k_own), (q_hbm, q_own), (v_hbm, v_own)))
        ]

    w_in = pltpu.make_async_copy(w_hbm, w_ref, bulk_sem.at[0])
    lat_in = pltpu.make_async_copy(lat_hbm, lat_ref, bulk_sem.at[1])

    def k_copy(h):
        return remote(k_hbm.at[:, columns(h)], k_prev.at[h], kv_ss.at[h, 0], kv_rs.at[h, 0], frame=f + 1)

    def v_copy(h):
        return remote(v_hbm.at[:, columns(h)], v_prev.at[h], kv_ss.at[h, 1], kv_rs.at[h, 1], frame=f + 1)

    def q_copy(h):
        return remote(q_hbm.at[:, columns(h)], q_guest.at[h], q_ss.at[h], q_rs.at[h], frame=f - 2)

    def o_copy(h):
        return remote(o_send.at[h], o_recv.at[h], o_ss.at[h], o_rs.at[h], frame=f + 2)

    def st_copy(h):
        return remote(st_send.at[h], st_recv.at[h], st_ss.at[h], st_rs.at[h], frame=f + 2)

    pen_copy = remote(pen_own, pen_guest, pen_sem.at[0], pen_sem.at[1], frame=f - 2)

    barrier = pltpu.get_barrier_semaphore()
    for there, step in ((has_prev, -1), (has_down, -2), (has_next, 1), (has_up, 2)):
        @pl.when(there)
        def _():
            pl.semaphore_signal(barrier, inc=1, device_id={"frame": f + step}, device_id_type=MESH)
    for peer in (pair, far):
        pl.semaphore_signal(barrier, inc=1, device_id={"head": peer}, device_id_type=MESH)

    for h in range(heads):
        for copy in local_in(h):
            copy.start()
    w_in.start()
    lat_in.start()

    for k in range(4):
        allowed = (mask_ref[0, k] == 1) & (f - k >= 0)
        pen_own[k:k + 1, :] = jnp.full((1, LANES), jnp.where(allowed, 0.0, FAR), f32)
    pen_own[4:, :] = jnp.zeros((4, LANES), f32)

    @pl.when(f == 0)
    def _():
        k_prev[...] = jnp.zeros_like(k_prev)
        v_prev[...] = jnp.zeros_like(v_prev)

    @pl.when(f < 2)
    def _():
        o_recv[...] = jnp.zeros_like(o_recv)
        st_recv[...] = jnp.full(st_recv.shape, LOW, f32)

    others = (
        2 + has_prev.astype(jnp.int32) + has_down.astype(jnp.int32)
        + has_next.astype(jnp.int32) + has_up.astype(jnp.int32)
    )
    pl.semaphore_wait(barrier, others)

    @pl.when(has_down)
    def _():
        pen_copy.start()
    for h in range(heads):
        @pl.when(has_next)
        def _():
            k_copy(h).start()
            v_copy(h).start()

        @pl.when(has_down)
        def _():
            q_copy(h).start()

    eye = lax.broadcasted_iota(jnp.int32, (LANES, LANES), 0) == lax.broadcasted_iota(
        jnp.int32, (LANES, LANES), 1
    )

    @pl.when(has_up)
    def _():
        pen_copy.wait_recv()

    def merge(h):
        @pl.when(has_down)
        def _():
            o_copy(h).wait_recv()
            st_copy(h).wait_recv()
        for a in range(span // LANES):
            rows = pl.ds(a * LANES, LANES)
            guest_lse = jnp.sum(
                jnp.where(eye, st_recv[h, a:a + 1, :], 0.0), axis=1, keepdims=True
            )
            share = 1.0 / (1.0 + jnp.exp2(lse_loc[h, rows, :] - guest_lse))
            mine = o_loc[h, rows, :]
            both = mine + share * (o_recv[h, rows, :].astype(f32) - mine)
            attended[rows, columns(h)] = both.astype(bf16)

    def one_head(h, carry):
        for copy in local_in(h):
            copy.wait()

        @pl.when(has_prev)
        def _():
            k_copy(h).wait_recv()
            v_copy(h).wait_recv()
        blocks = ((k_own[h], v_own[h]), (k_prev[h], v_prev[h]))

        @pl.when(has_up)
        def _():
            q_copy(h).wait_recv()
            for t in range(span // tile):
                rows = pl.ds(t * tile, tile)
                out, lse = partial_attention(
                    q_guest[h, rows, :], blocks, (pen_guest[2:3, 0:1], pen_guest[3:4, 0:1])
                )
                o_send[h, rows, :] = out.astype(bf16)
                for a in range(tile // LANES):
                    at = t * (tile // LANES) + a
                    st_send[h, at:at + 1, :] = jnp.sum(
                        jnp.where(eye, lse[a * LANES:(a + 1) * LANES, :], 0.0), axis=0, keepdims=True
                    )
            o_copy(h).start()
            st_copy(h).start()

        for t in range(span // tile):
            rows = pl.ds(t * tile, tile)
            out, lse = partial_attention(
                q_own[h, rows, :], blocks, (pen_own[0:1, 0:1], pen_own[1:2, 0:1])
            )
            o_loc[h, rows, :] = out
            lse_loc[h, rows, :] = lse

        @pl.when(h >= 1)
        def _():
            merge(h - 1)
        return carry

    lax.fori_loop(0, heads, one_head, 0)
    merge(heads - 1)

    w_in.wait()
    lat_in.wait()
    level = jnp.full((1, LANES), levels_ref[0], jnp.int32).astype(f32)
    delta = (noise_level(level / LEVELS) - noise_level((level + 1.0) / LEVELS))[:, 0:1]
    gate = jnp.zeros((1, out_width), f32)
    for n in range(LEVELS):
        gate = gate + jnp.where(level[:, 0:1] == float(n), gate_ref[n:n + 1, :], 0.0)
    gate_row[...] = gate

    def at_rows(i):
        return pl.ds(pl.multiple_of((i % row_parts) * prow, prow), prow)

    def at_cols(i, base=0):
        return pl.ds(pl.multiple_of(base + (i // row_parts) * pcol, LANES), pcol)

    def project(i, owner):
        return jnp.dot(
            attended[at_rows(i), :], w_ref[:, at_cols(i, owner * out_width)],
            preferred_element_type=f32,
        )

    def pair_copy(i):
        return remote(pair_send.at[i], pair_recv.at[i], pair_ss.at[i], pair_rs.at[i], head=pair)

    def near_copy(i):
        return remote(near_send.at[i], near_recv.at[i], near_ss.at[i], near_rs.at[i], head=pair)

    def far_copy(i):
        return remote(far_send.at[i], far_recv.at[i], far_ss.at[i], far_rs.at[i], head=far)

    def slide_copy(i):
        return remote(
            upd_stage.at[i], next_hbm.at[at_rows(i), at_cols(i)], slide_ss.at[i], slide_rs.at[i],
            frame=f - 1,
        )

    def vel_copy(i):
        return pltpu.make_async_copy(
            vel_stage.at[i], vel_hbm.at[at_rows(i), at_cols(i)], vel_sem.at[i]
        )

    diagonal = (pair + 2) % 4

    def send_pair(i):
        pair_send[i] = project(i, diagonal).astype(bf16)
        pair_copy(i).start()

    send_pair(0)

    def exchange(i, carry):
        @pl.when(i + 1 < pieces)
        def _():
            send_pair(i + 1)
        mine = project(i, far)
        pair_copy(i).wait_recv()
        far_send[i] = (mine.astype(bf16).astype(f32) + pair_recv[i].astype(f32)).astype(bf16)
        far_copy(i).start()
        return carry

    lax.fori_loop(0, pieces, exchange, 0)

    def send_near(i, carry):
        near_send[i] = project(i, pair).astype(bf16)
        near_copy(i).start()
        return carry

    lax.fori_loop(0, pieces, send_near, 0)

    def join(i, carry):
        total = project(i, me).astype(bf16).astype(f32)
        near_copy(i).wait_recv()
        far_copy(i).wait_recv()
        total = total + near_recv[i].astype(f32) + far_recv[i].astype(f32)
        gated = gate_row[0:1, at_cols(i)] * total
        upd_stage[i] = (lat_ref[at_rows(i), at_cols(i)].astype(f32) + delta * gated).astype(bf16)

        @pl.when(has_prev)
        def _():
            slide_copy(i).start()
        vel_stage[i] = gated.astype(bf16)
        vel_copy(i).start()
        return carry

    lax.fori_loop(0, pieces, join, 0)

    for h in range(heads):
        @pl.when(has_next)
        def _():
            k_copy(h).wait_send()
            v_copy(h).wait_send()

        @pl.when(has_down)
        def _():
            q_copy(h).wait_send()

        @pl.when(has_up)
        def _():
            o_copy(h).wait_send()
            st_copy(h).wait_send()

    @pl.when(has_down)
    def _():
        pen_copy.wait_send()

    @pl.when(f == frames - 1)
    def _():
        fresh_in = pltpu.make_async_copy(fresh_hbm, lat_ref, bulk_sem.at[0])
        fresh_in.start()
        fresh_in.wait()
        fresh_out = pltpu.make_async_copy(lat_ref, next_hbm, bulk_sem.at[1])
        fresh_out.start()
        fresh_out.wait()

    def drain(i, carry):
        pair_copy(i).wait_send()
        near_copy(i).wait_send()
        far_copy(i).wait_send()
        vel_copy(i).wait()

        @pl.when(has_prev)
        def _():
            slide_copy(i).wait_send()

        @pl.when(has_next)
        def _():
            slide_copy(i).wait_recv()
        return carry

    lax.fori_loop(0, pieces, drain, 0)


def shards(latents, queries, keys, values, out_weight, gate_table, levels, block_mask, fresh):
    span, hh = queries.shape
    heads = hh // HD
    out_width = latents.shape[1]
    assert lax.axis_size("head") == 4 and block_mask.shape[1] == 4
    assert out_weight.shape[1] == 4 * out_width
    prow = span // 2
    pcol = 2 * LANES if out_width % (2 * LANES) == 0 else LANES
    pieces = (span // prow) * (out_width // pcol)

    vmem = pltpu.VMEM
    dma = pltpu.SemaphoreType.DMA
    head_block = vmem((heads, span, HD), bf16)
    head_wide = vmem((heads, span, HD), f32)
    stats = vmem((heads, 8, LANES), f32)
    piece = vmem((pieces, prow, pcol), bf16)
    any_spec = pl.BlockSpec(memory_space=pl.ANY)
    out = jax.ShapeDtypeStruct((span, out_width), bf16)
    return pl.pallas_call(
        kernel,
        in_specs=[pl.BlockSpec(memory_space=pltpu.SMEM)] * 2 + [any_spec] * 6
        + [pl.BlockSpec(memory_space=pltpu.VMEM)],
        out_specs=[any_spec, any_spec],
        out_shape=[out, out],
        scratch_shapes=[head_block] * 6
        + [vmem((8, LANES), f32)] * 2
        + [head_block, head_block, stats, stats, head_wide, head_wide]
        + [vmem((span, hh), bf16), vmem(out_weight.shape, bf16), vmem((span, out_width), bf16)]
        + [vmem((1, out_width), f32)]
        + [piece] * 8
        + [dma((heads, 3)), dma((2,)), dma((heads, 2)), dma((heads, 2))]
        + [dma((heads,))] * 6
        + [dma((2,))]
        + [dma((pieces,))] * 9,
        compiler_params=pltpu.CompilerParams(
            collective_id=0, has_side_effects=True, vmem_limit_bytes=60 * 1024 * 1024
        ),
    )(levels, block_mask, queries, keys, values, out_weight, latents, fresh, gate_table)


def solution(mesh):
    in_specs = (
        P("frame", "head"),
        P("frame", "head"),
        P("frame", "head"),
        P("frame", "head"),
        P("head", None),
        P(None, "head"),
        P("frame"),
        P("frame", None),
        P(None, "head"),
    )
    out_specs = (P("frame", "head"), P("frame", "head"))
    return jax.shard_map(shards, mesh=mesh, in_specs=in_specs, out_specs=out_specs, check_vma=False)
```

```python
import functools
import math

import jax
import jax.numpy as jnp
from jax import lax
from jax.experimental import pallas as pl
from jax.experimental.pallas import tpu as pltpu
from jax.sharding import PartitionSpec as P

HD = 128
LANES = 128
LEVELS = 4
FAR = 1e30
LOW = -1e20
VMEM_LIMIT = 60 * 1024 * 1024

flow_shift = 5.0

MESH = pl.DeviceIdType.MESH
bf16 = jnp.bfloat16
f32 = jnp.float32


def noise_level(point):
    return flow_shift * point / (1.0 + (flow_shift - 1.0) * point)


def scores_of(query, keys):
    scale = math.log2(math.e) / math.sqrt(HD)
    return lax.dot_general(query, keys, (((1,), (1,)), ((), ())), preferred_element_type=f32) * scale


def with_ones(values):
    return jnp.concatenate([values, jnp.ones((values.shape[0], LANES), bf16)], axis=1)


def kernel(
    levels_hbm, mask_hbm, q_hbm, k_hbm, v_hbm, w_hbm, lat_hbm, fresh_hbm, gate_hbm,
    vel_hbm, next_hbm,
    levels_ref, mask_ref, gate_ref,
    q_own, k_own, v_own, q_guest, k_prev, v_prev, v_relay, pen_own, pen_guest,
    acc_ref, top_ref, p_ref,
    o_send, o_recv, st_send, st_recv, o_loc, lse_loc, attended, w_ref, lat_ref, gate_row,
    pair_send, pair_recv, near_send, near_recv, far_send, far_recv, vel_stage, upd_stage,
    in_sem, bulk_sem, kv_ss, kv_rs, relay_ss, relay_rs, q_ss, q_rs, o_ss, o_rs, st_ss, st_rs, pen_sem,
    pair_ss, pair_rs, near_ss, near_rs, far_ss, far_rs, vel_sem, slide_ss, slide_rs,
):
    f = lax.axis_index("frame")
    frames = lax.axis_size("frame")
    me = lax.axis_index("head")
    heads, span, _ = q_own.shape
    pieces, prow, pcol = pair_send.shape
    row_parts = span // prow
    col_parts = pieces // row_parts
    out_width = lat_ref.shape[1]
    tile = prow
    tiles = span // tile
    lag = min(3, pieces)

    pair = me + 1 - 2 * (me % 2)
    far = (me + 2) % 4
    odd = f % 2 == 1
    even = f % 2 == 0
    has_prev = f >= 1
    has_down = f >= 2
    has_next = f + 1 < frames
    has_up = f + 2 < frames

    def remote(src, dst, ss, rs, frame=None, head=None):
        where = {"frame": frame} if head is None else {"head": head}
        return pltpu.make_async_remote_copy(
            src_ref=src, dst_ref=dst, send_sem=ss, recv_sem=rs, device_id=where, device_id_type=MESH
        )

    def columns(h):
        return pl.ds(pl.multiple_of(h * HD, HD), HD)

    def local_in(h):
        return [
            pltpu.make_async_copy(src.at[:, columns(h)], dst.at[h], in_sem.at[h, i])
            for i, (src, dst) in enumerate(((k_hbm, k_own), (q_hbm, q_own), (v_hbm, v_own)))
        ]

    w_in = pltpu.make_async_copy(w_hbm, w_ref, bulk_sem.at[0])
    lat_in = pltpu.make_async_copy(lat_hbm, lat_ref, bulk_sem.at[1])
    mask_in = pltpu.make_async_copy(mask_hbm, mask_ref, bulk_sem.at[2])
    levels_in = pltpu.make_async_copy(levels_hbm, levels_ref, bulk_sem.at[3])
    gate_in = pltpu.make_async_copy(gate_hbm, gate_ref, bulk_sem.at[4])

    def k_copy(h):
        return remote(k_hbm.at[:, columns(h)], k_prev.at[h], kv_ss.at[h, 0], kv_rs.at[h, 0], frame=f + 1)

    def v_copy(h):
        return remote(v_hbm.at[:, columns(h)], v_prev.at[h], kv_ss.at[h, 1], kv_rs.at[h, 1], frame=f + 1)

    def relay_in(h):
        return remote(
            v_hbm.at[:, columns(h)], v_relay.at[h], relay_ss.at[h], relay_rs.at[h], frame=f - 1
        )

    def relay_out(h):
        return remote(v_relay.at[h], v_prev.at[h], kv_ss.at[h, 1], kv_rs.at[h, 1], frame=f + 2)

    def q_copy(h):
        return remote(q_hbm.at[:, columns(h)], q_guest.at[h], q_ss.at[h], q_rs.at[h], frame=f - 2)

    def o_copy(h, t):
        rows = pl.ds(t * tile, tile)
        return remote(
            o_send.at[h, rows], o_recv.at[h, rows], o_ss.at[h, t], o_rs.at[h, t], frame=f + 2
        )

    def st_copy(h, t):
        return remote(st_send.at[h, t], st_recv.at[h, t], st_ss.at[h, t], st_rs.at[h, t], frame=f + 2)

    pen_copy = remote(pen_own, pen_guest, pen_sem.at[0], pen_sem.at[1], frame=f - 2)

    barrier = pltpu.get_barrier_semaphore()
    for there, step in ((has_prev, -1), (has_down, -2), (has_next, 1), (has_up, 2)):
        @pl.when(there)
        def _():
            pl.semaphore_signal(barrier, inc=1, device_id={"frame": f + step}, device_id_type=MESH)
    for peer in (pair, far):
        pl.semaphore_signal(barrier, inc=1, device_id={"head": peer}, device_id_type=MESH)

    mask_in.start()
    for h in range(heads):
        for copy in local_in(h):
            copy.start()

    @pl.when(f == 0)
    def _():
        k_prev[...] = jnp.zeros_like(k_prev)
        v_prev[...] = jnp.zeros_like(v_prev)

    @pl.when(f < 2)
    def _():
        o_recv[...] = jnp.zeros_like(o_recv)
        st_recv[...] = jnp.full(st_recv.shape, LOW, f32)

    @pl.when(f + 2 >= frames)
    def _():
        q_guest[...] = jnp.zeros_like(q_guest)
        pen_guest[...] = jnp.zeros_like(pen_guest)

    others = (
        2 + has_prev.astype(jnp.int32) + has_down.astype(jnp.int32)
        + has_next.astype(jnp.int32) + has_up.astype(jnp.int32)
    )
    pl.semaphore_wait(barrier, others)

    @pl.when(even & has_next)
    def _():
        for h in range(heads):
            k_copy(h).start()
            v_copy(h).start()

    @pl.when(odd & has_next)
    def _():
        for h in range(heads):
            relay_in(h).start()

    @pl.when(has_down)
    def _():
        for h in range(heads):
            q_copy(h).start()

    w_in.start()
    levels_in.start()
    gate_in.start()
    lat_in.start()

    mask_in.wait()
    for k in range(4):
        allowed = (mask_ref[0, k] == 1) & (f - k >= 0)
        pen_own[k:k + 1, :] = jnp.full((1, LANES), jnp.where(allowed, 0.0, FAR), f32)
    pen_own[4:, :] = jnp.zeros((4, LANES), f32)

    @pl.when(has_down)
    def _():
        pen_copy.start()

    @pl.when(odd & has_next)
    def _():
        relay_in(0).wait_send()
        for h in range(heads):
            k_copy(h).start()

    eye = lax.broadcasted_iota(jnp.int32, (LANES, LANES), 0) == lax.broadcasted_iota(
        jnp.int32, (LANES, LANES), 1
    )

    def merge(h, t):
        @pl.when(has_down)
        def _():
            o_copy(h, t).wait_recv()
            st_copy(h, t).wait_recv()
        for a in range(tile // LANES):
            rows = pl.ds(t * tile + a * LANES, LANES)
            guest_lse = jnp.sum(
                jnp.where(eye, st_recv[h, t, a:a + 1, :], 0.0), axis=1, keepdims=True
            )
            share = 1.0 / (1.0 + jnp.exp2(lse_loc[h, rows, :] - guest_lse))
            mine = o_loc[h, rows, :]
            both = mine + share * (o_recv[h, rows, :].astype(f32) - mine)
            attended[rows, columns(h)] = both.astype(bf16)

    @pl.when(has_up)
    def _():
        pen_copy.wait_recv()

    def forward(h):
        @pl.when(even & has_up)
        def _():
            relay_in(h).wait_recv()
            relay_out(h).start()

    forward(0)

    row_tiles = [(q_guest, pen_guest, 2, t, True) for t in range(tiles)]
    row_tiles += [(q_own, pen_own, 0, t, False) for t in range(tiles)]

    def one_head(h, carry):
        for copy in local_in(h):
            copy.wait()

        @pl.when(has_up)
        def _():
            q_copy(h).wait_recv()

        own_wide = with_ones(v_own[h])
        for n, (q_ref, pen_ref, first, t, _) in enumerate(row_tiles):
            at = pl.ds(n * tile, tile)
            s = scores_of(q_ref[h, pl.ds(t * tile, tile), :], k_own[h])
            penalty = pen_ref[first:first + 1, 0:1]
            top = jnp.maximum(jnp.max(s, axis=1, keepdims=True) - penalty, LOW)
            weights = jnp.exp2(s - (top + penalty)).astype(bf16)
            acc_ref[at, :] = jnp.dot(weights, own_wide, preferred_element_type=f32)
            top_ref[at, :] = top

        @pl.when(h >= 1)
        def _():
            for t in range(tiles):
                merge(h - 1, t)

        @pl.when(has_prev)
        def _():
            k_copy(h).wait_recv()

        @pl.when(h + 1 < heads)
        def _():
            forward(h + 1)

        for n, (q_ref, pen_ref, first, t, _) in enumerate(row_tiles):
            at = pl.ds(n * tile, tile)
            s = scores_of(q_ref[h, pl.ds(t * tile, tile), :], k_prev[h])
            penalty = pen_ref[first + 1:first + 2, 0:1]
            before = top_ref[at, :]
            top = jnp.maximum(jnp.max(s, axis=1, keepdims=True) - penalty, before)
            p_ref[at, :] = jnp.exp2(s - (top + penalty)).astype(bf16)
            acc_ref[at, :] = acc_ref[at, :] * jnp.exp2(before - top)
            top_ref[at, :] = top

        @pl.when(has_prev)
        def _():
            v_copy(h).wait_recv()

        prev_wide = with_ones(v_prev[h])
        for n, (_, _, _, t, guest) in enumerate(row_tiles):
            at = pl.ds(n * tile, tile)
            acc = acc_ref[at, :] + jnp.dot(p_ref[at, :], prev_wide, preferred_element_type=f32)
            total = jnp.maximum(acc[:, HD:], 1.0)
            out = acc[:, :HD] / total
            lse = top_ref[at, :] + jnp.log2(total)
            rows = pl.ds(t * tile, tile)
            if guest:
                o_send[h, rows, :] = out.astype(bf16)
                for a in range(tile // LANES):
                    st_send[h, t, a:a + 1, :] = jnp.sum(
                        jnp.where(eye, lse[a * LANES:(a + 1) * LANES, :], 0.0), axis=0, keepdims=True
                    )

                @pl.when(has_up)
                def _():
                    o_copy(h, t).start()
                    st_copy(h, t).start()
            else:
                o_loc[h, rows, :] = out
                lse_loc[h, rows, :] = lse
        return carry

    lax.fori_loop(0, heads, one_head, 0)

    w_in.wait()
    lat_in.wait()
    levels_in.wait()
    gate_in.wait()
    level = jnp.full((1, LANES), levels_ref[0], jnp.int32).astype(f32)
    delta = (noise_level(level / LEVELS) - noise_level((level + 1.0) / LEVELS))[:, 0:1]
    gate = jnp.zeros((1, out_width), f32)
    for n in range(LEVELS):
        gate = gate + jnp.where(level[:, 0:1] == float(n), gate_ref[n:n + 1, :], 0.0)
    gate_row[...] = gate

    def at_rows(i):
        return pl.ds(pl.multiple_of((i // col_parts) * prow, prow), prow)

    def at_cols(i, base=0):
        return pl.ds(pl.multiple_of(base + (i % col_parts) * pcol, LANES), pcol)

    def project(i, owner):
        return jnp.dot(
            attended[at_rows(i), :], w_ref[:, at_cols(i, owner * out_width)],
            preferred_element_type=f32,
        )

    def pair_copy(i):
        return remote(pair_send.at[i], pair_recv.at[i], pair_ss.at[i], pair_rs.at[i], head=pair)

    def near_copy(i):
        return remote(near_send.at[i], near_recv.at[i], near_ss.at[i], near_rs.at[i], head=pair)

    def far_copy(i):
        return remote(far_send.at[i], far_recv.at[i], far_ss.at[i], far_rs.at[i], head=far)

    def slide_copy(i):
        return remote(
            upd_stage.at[i], next_hbm.at[at_rows(i), at_cols(i)], slide_ss.at[i], slide_rs.at[i],
            frame=f - 1,
        )

    def vel_copy(i):
        return pltpu.make_async_copy(
            vel_stage.at[i], vel_hbm.at[at_rows(i), at_cols(i)], vel_sem.at[i]
        )

    diagonal = (pair + 2) % 4

    def send_pair(i):
        pair_send[i] = project(i, diagonal).astype(bf16)
        pair_copy(i).start()

    merge(heads - 1, 0)
    send_pair(0)

    def exchange(i, carry):
        for t in range(1, row_parts):
            @pl.when(i == t * col_parts - 2)
            def _():
                merge(heads - 1, t)

        @pl.when(i + 1 < pieces)
        def _():
            send_pair(i + 1)

        @pl.when(i < pieces)
        def _():
            mine = project(i, far)
            pair_copy(i).wait_recv()
            far_send[i] = (mine.astype(bf16).astype(f32) + pair_recv[i].astype(f32)).astype(bf16)
            far_copy(i).start()
            near_send[i] = project(i, pair).astype(bf16)
            near_copy(i).start()

        @pl.when(i >= lag)
        def _():
            join(i - lag)
        return carry

    def join(i):
        total = project(i, me).astype(bf16).astype(f32)
        near_copy(i).wait_recv()
        far_copy(i).wait_recv()
        total = total + near_recv[i].astype(f32) + far_recv[i].astype(f32)
        gated = gate_row[0:1, at_cols(i)] * total
        upd_stage[i] = (lat_ref[at_rows(i), at_cols(i)].astype(f32) + delta * gated).astype(bf16)

        @pl.when(has_prev)
        def _():
            slide_copy(i).start()
        vel_stage[i] = gated.astype(bf16)
        vel_copy(i).start()

    lax.fori_loop(0, pieces + lag, exchange, 0)

    for h in range(heads):
        @pl.when(has_next)
        def _():
            k_copy(h).wait_send()

        @pl.when(even & has_next)
        def _():
            v_copy(h).wait_send()

        @pl.when(has_down)
        def _():
            q_copy(h).wait_send()

        @pl.when(has_up)
        def _():
            for t in range(tiles):
                o_copy(h, t).wait_send()
                st_copy(h, t).wait_send()

    @pl.when(odd & has_next)
    def _():
        for h in range(1, heads):
            relay_in(h).wait_send()

    @pl.when(even & has_up)
    def _():
        for h in range(heads):
            relay_out(h).wait_send()

    @pl.when(has_down)
    def _():
        pen_copy.wait_send()

    @pl.when(f == frames - 1)
    def _():
        fresh_in = pltpu.make_async_copy(fresh_hbm, lat_ref, bulk_sem.at[0])
        fresh_in.start()
        fresh_in.wait()
        fresh_out = pltpu.make_async_copy(lat_ref, next_hbm, bulk_sem.at[1])
        fresh_out.start()
        fresh_out.wait()

    def drain(i, carry):
        pair_copy(i).wait_send()
        near_copy(i).wait_send()
        far_copy(i).wait_send()
        vel_copy(i).wait()

        @pl.when(has_prev)
        def _():
            slide_copy(i).wait_send()

        @pl.when(has_next)
        def _():
            slide_copy(i).wait_recv()
        return carry

    lax.fori_loop(0, pieces, drain, 0)


def shards(latents, queries, keys, values, out_weight, gate_table, levels, block_mask, fresh):
    span, hh = queries.shape
    heads = hh // HD
    out_width = latents.shape[1]
    assert lax.axis_size("head") == 4 and block_mask.shape[1] == 4
    assert out_weight.shape[1] == 4 * out_width
    prow = span // 2
    pcol = 2 * LANES if out_width % (2 * LANES) == 0 else LANES
    pieces = (span // prow) * (out_width // pcol)

    vmem = pltpu.VMEM
    dma = pltpu.SemaphoreType.DMA
    tiles = span // prow
    head_block = vmem((heads, span, HD), bf16)
    head_wide = vmem((heads, span, HD), f32)
    stats = vmem((heads, tiles, 8, LANES), f32)
    piece = vmem((pieces, prow, pcol), bf16)
    any_spec = pl.BlockSpec(memory_space=pl.ANY)
    out = jax.ShapeDtypeStruct((span, out_width), bf16)
    return pl.pallas_call(
        kernel,
        in_specs=[any_spec] * 9,
        out_specs=[any_spec, any_spec],
        out_shape=[out, out],
        scratch_shapes=[pltpu.SMEM((1,), jnp.int32), pltpu.SMEM((1, 4), jnp.int32)]
        + [vmem(gate_table.shape, f32)]
        + [head_block] * 7
        + [vmem((8, LANES), f32)] * 2
        + [vmem((2 * span, 2 * HD), f32), vmem((2 * span, 1), f32), vmem((2 * span, span), bf16)]
        + [head_block, head_block, stats, stats, head_wide, head_wide]
        + [vmem((span, hh), bf16), vmem(out_weight.shape, bf16), vmem((span, out_width), bf16)]
        + [vmem((1, out_width), f32)]
        + [piece] * 8
        + [dma((heads, 3)), dma((5,)), dma((heads, 2)), dma((heads, 2))]
        + [dma((heads,))] * 4
        + [dma((heads, tiles))] * 4
        + [dma((2,))]
        + [dma((pieces,))] * 9,
        compiler_params=pltpu.CompilerParams(
            collective_id=0, has_side_effects=True, vmem_limit_bytes=VMEM_LIMIT
        ),
    )(
        levels, block_mask, queries, keys, values, out_weight, latents, fresh, gate_table
    )


def solution(mesh):
    in_specs = (
        P("frame", "head"),
        P("frame", "head"),
        P("frame", "head"),
        P("frame", "head"),
        P("head", None),
        P(None, "head"),
        P("frame"),
        P("frame", None),
        P(None, "head"),
    )
    out_specs = (P("frame", "head"), P("frame", "head"))
    return jax.shard_map(shards, mesh=mesh, in_specs=in_specs, out_specs=out_specs, check_vma=False)
```

```python
import functools
import math

import jax
import jax.numpy as jnp
from jax import lax
from jax.experimental import pallas as pl
from jax.experimental.pallas import tpu as pltpu
from jax.sharding import PartitionSpec as P

HD = 128
LANES = 128
LEVELS = 4
FAR = 1e30
LOW = -1e20
VMEM_LIMIT = 60 * 1024 * 1024

flow_shift = 5.0

MESH = pl.DeviceIdType.MESH
bf16 = jnp.bfloat16
f32 = jnp.float32


def noise_level(point):
    return flow_shift * point / (1.0 + (flow_shift - 1.0) * point)


def scores_of(query, keys):
    scale = math.log2(math.e) / math.sqrt(HD)
    return lax.dot_general(query, keys, (((1,), (1,)), ((), ())), preferred_element_type=f32) * scale


def with_ones(values):
    return jnp.concatenate([values, jnp.ones((values.shape[0], LANES), bf16)], axis=1)


def kernel(
    levels_hbm, mask_hbm, q_hbm, k_hbm, v_hbm, w_hbm, lat_hbm, fresh_hbm, gate_hbm,
    vel_hbm, next_hbm,
    levels_ref, mask_ref, gate_ref,
    q_own, k_own, v_own, q_guest, k_prev, v_prev, relay, pen_own, pen_guest,
    acc_ref, top_ref, p_ref,
    o_send, o_recv, st_send, st_recv, o_loc, lse_loc, attended, w_ref, lat_ref, gate_row,
    pair_send, pair_recv, near_send, near_recv, far_send, far_recv, vel_stage, upd_stage,
    in_sem, bulk_sem, kv_ss, kv_rs, relay_ss, relay_rs, fwd_ss, q_ss, q_rs, o_ss, o_rs, st_ss, st_rs, pen_sem,
    pair_ss, pair_rs, near_ss, near_rs, far_ss, far_rs, vel_sem, slide_ss, slide_rs,
):
    f = lax.axis_index("frame")
    frames = lax.axis_size("frame")
    me = lax.axis_index("head")
    heads, span, _ = q_own.shape
    pieces, prow, pcol = pair_send.shape
    row_parts = span // prow
    col_parts = pieces // row_parts
    out_width = lat_ref.shape[1]
    tile = prow
    tiles = span // tile
    lag = min(3, pieces)

    pair = me + 1 - 2 * (me % 2)
    far = (me + 2) % 4
    odd = f % 2 == 1
    even = f % 2 == 0
    has_prev = f >= 1
    has_down = f >= 2
    has_next = f + 1 < frames
    has_up = f + 2 < frames

    def remote(src, dst, ss, rs, frame=None, head=None):
        where = {"frame": frame} if head is None else {"head": head}
        return pltpu.make_async_remote_copy(
            src_ref=src, dst_ref=dst, send_sem=ss, recv_sem=rs, device_id=where, device_id_type=MESH
        )

    def columns(h):
        return pl.ds(pl.multiple_of(h * HD, HD), HD)

    def local_in(h):
        return [
            pltpu.make_async_copy(src.at[:, columns(h)], dst.at[h], in_sem.at[h, i])
            for i, (src, dst) in enumerate(((k_hbm, k_own), (q_hbm, q_own), (v_hbm, v_own)))
        ]

    w_in = pltpu.make_async_copy(w_hbm, w_ref, bulk_sem.at[0])
    lat_in = pltpu.make_async_copy(lat_hbm, lat_ref, bulk_sem.at[1])
    mask_in = pltpu.make_async_copy(mask_hbm, mask_ref, bulk_sem.at[2])
    levels_in = pltpu.make_async_copy(levels_hbm, levels_ref, bulk_sem.at[3])
    gate_in = pltpu.make_async_copy(gate_hbm, gate_ref, bulk_sem.at[4])

    def k_copy(h):
        return remote(k_hbm.at[:, columns(h)], k_prev.at[h], kv_ss.at[h, 0], kv_rs.at[h, 0], frame=f + 1)

    def v_copy(h):
        return remote(v_hbm.at[:, columns(h)], v_prev.at[h], kv_ss.at[h, 1], kv_rs.at[h, 1], frame=f + 1)

    def relay_keys(h):
        return remote(
            k_hbm.at[:, columns(h)], relay.at[h], relay_ss.at[h, 0], relay_rs.at[h], frame=f - 1
        )

    def relay_values(h):
        return remote(
            v_hbm.at[:, columns(h)], relay.at[h], relay_ss.at[h, 1], relay_rs.at[h], frame=f + 2
        )

    def forward_keys(h):
        return remote(relay.at[h], k_prev.at[h], fwd_ss.at[h], kv_rs.at[h, 0], frame=f + 2)

    def forward_values(h):
        return remote(relay.at[h], v_prev.at[h], fwd_ss.at[h], kv_rs.at[h, 1], frame=f - 1)

    def q_copy(h):
        return remote(q_hbm.at[:, columns(h)], q_guest.at[h], q_ss.at[h], q_rs.at[h], frame=f - 2)

    def o_copy(h, t):
        rows = pl.ds(t * tile, tile)
        return remote(
            o_send.at[h, rows], o_recv.at[h, rows], o_ss.at[h, t], o_rs.at[h, t], frame=f + 2
        )

    def st_copy(h, t):
        return remote(st_send.at[h, t], st_recv.at[h, t], st_ss.at[h, t], st_rs.at[h, t], frame=f + 2)

    pen_copy = remote(pen_own, pen_guest, pen_sem.at[0], pen_sem.at[1], frame=f - 2)

    barrier = pltpu.get_barrier_semaphore()
    for there, step in ((has_prev, -1), (has_down, -2), (has_next, 1), (has_up, 2)):
        @pl.when(there)
        def _():
            pl.semaphore_signal(barrier, inc=1, device_id={"frame": f + step}, device_id_type=MESH)
    for peer in (pair, far):
        pl.semaphore_signal(barrier, inc=1, device_id={"head": peer}, device_id_type=MESH)

    mask_in.start()
    for h in range(heads):
        for copy in local_in(h):
            copy.start()

    @pl.when(f == 0)
    def _():
        k_prev[...] = jnp.zeros_like(k_prev)
        v_prev[...] = jnp.zeros_like(v_prev)

    @pl.when(f < 2)
    def _():
        o_recv[...] = jnp.zeros_like(o_recv)
        st_recv[...] = jnp.full(st_recv.shape, LOW, f32)

    @pl.when(f + 2 >= frames)
    def _():
        q_guest[...] = jnp.zeros_like(q_guest)
        pen_guest[...] = jnp.zeros_like(pen_guest)

    mask_in.wait()
    for k in range(4):
        allowed = (mask_ref[0, k] == 1) & (f - k >= 0)
        pen_own[k:k + 1, :] = jnp.full((1, LANES), jnp.where(allowed, 0.0, FAR), f32)
    pen_own[4:, :] = jnp.zeros((4, LANES), f32)

    others = (
        2 + has_prev.astype(jnp.int32) + has_down.astype(jnp.int32)
        + has_next.astype(jnp.int32) + has_up.astype(jnp.int32)
    )
    pl.semaphore_wait(barrier, others)

    @pl.when(even & has_next)
    def _():
        for h in range(heads):
            k_copy(h).start()
            v_copy(h).start()

    @pl.when(odd & has_next)
    def _():
        for h in range(heads):
            relay_values(h).start()
        for h in range(2):
            relay_keys(h).start()

    @pl.when(has_down)
    def _():
        pen_copy.start()
        for h in range(heads):
            q_copy(h).start()

    w_in.start()
    levels_in.start()
    gate_in.start()
    lat_in.start()

    eye = lax.broadcasted_iota(jnp.int32, (LANES, LANES), 0) == lax.broadcasted_iota(
        jnp.int32, (LANES, LANES), 1
    )

    def merge(h, t):
        @pl.when(has_down)
        def _():
            o_copy(h, t).wait_recv()
            st_copy(h, t).wait_recv()
        for a in range(tile // LANES):
            rows = pl.ds(t * tile + a * LANES, LANES)
            guest_lse = jnp.sum(
                jnp.where(eye, st_recv[h, t, a:a + 1, :], 0.0), axis=1, keepdims=True
            )
            share = 1.0 / (1.0 + jnp.exp2(lse_loc[h, rows, :] - guest_lse))
            mine = o_loc[h, rows, :]
            both = mine + share * (o_recv[h, rows, :].astype(f32) - mine)
            attended[rows, columns(h)] = both.astype(bf16)

    @pl.when(has_up)
    def _():
        pen_copy.wait_recv()

    def forward(h):
        @pl.when(even & has_up)
        def _():
            relay_keys(h).wait_recv()
            forward_keys(h).start()

        @pl.when(odd & has_down)
        def _():
            relay_values(h).wait_recv()
            forward_values(h).start()

        @pl.when(odd & has_next & (h + 2 < heads))
        def _():
            relay_keys(h + 2).start()

    forward(0)

    row_tiles = [(q_guest, pen_guest, 2, t, True) for t in range(tiles)]
    row_tiles += [(q_own, pen_own, 0, t, False) for t in range(tiles)]

    def one_head(h, carry):
        for copy in local_in(h):
            copy.wait()

        @pl.when(has_up)
        def _():
            q_copy(h).wait_recv()

        own_wide = with_ones(v_own[h])
        for n, (q_ref, pen_ref, first, t, _) in enumerate(row_tiles):
            at = pl.ds(n * tile, tile)
            s = scores_of(q_ref[h, pl.ds(t * tile, tile), :], k_own[h])
            penalty = pen_ref[first:first + 1, 0:1]
            top = jnp.maximum(jnp.max(s, axis=1, keepdims=True) - penalty, LOW)
            weights = jnp.exp2(s - (top + penalty)).astype(bf16)
            acc_ref[at, :] = jnp.dot(weights, own_wide, preferred_element_type=f32)
            top_ref[at, :] = top

        @pl.when(h + 1 < heads)
        def _():
            forward(h + 1)

        @pl.when(has_prev)
        def _():
            k_copy(h).wait_recv()

        for n, (q_ref, pen_ref, first, t, _) in enumerate(row_tiles):
            at = pl.ds(n * tile, tile)
            s = scores_of(q_ref[h, pl.ds(t * tile, tile), :], k_prev[h])
            penalty = pen_ref[first + 1:first + 2, 0:1]
            before = top_ref[at, :]
            top = jnp.maximum(jnp.max(s, axis=1, keepdims=True) - penalty, before)
            p_ref[at, :] = jnp.exp2(s - (top + penalty)).astype(bf16)
            acc_ref[at, :] = acc_ref[at, :] * jnp.exp2(before - top)
            top_ref[at, :] = top

        @pl.when(has_prev)
        def _():
            v_copy(h).wait_recv()

        prev_wide = with_ones(v_prev[h])
        for n, (_, _, _, t, guest) in enumerate(row_tiles):
            at = pl.ds(n * tile, tile)
            acc = acc_ref[at, :] + jnp.dot(p_ref[at, :], prev_wide, preferred_element_type=f32)
            total = jnp.maximum(acc[:, HD:], 1.0)
            out = acc[:, :HD] / total
            lse = top_ref[at, :] + jnp.log2(total)
            rows = pl.ds(t * tile, tile)
            if guest:
                o_send[h, rows, :] = out.astype(bf16)
                for a in range(tile // LANES):
                    st_send[h, t, a:a + 1, :] = jnp.sum(
                        jnp.where(eye, lse[a * LANES:(a + 1) * LANES, :], 0.0), axis=0, keepdims=True
                    )

                @pl.when(has_up)
                def _():
                    o_copy(h, t).start()
                    st_copy(h, t).start()
            else:
                o_loc[h, rows, :] = out
                lse_loc[h, rows, :] = lse
        return carry

    lax.fori_loop(0, heads, one_head, 0)

    w_in.wait()
    lat_in.wait()
    levels_in.wait()
    gate_in.wait()
    level = jnp.full((1, LANES), levels_ref[0], jnp.int32).astype(f32)
    delta = (noise_level(level / LEVELS) - noise_level((level + 1.0) / LEVELS))[:, 0:1]
    gate = jnp.zeros((1, out_width), f32)
    for n in range(LEVELS):
        gate = gate + jnp.where(level[:, 0:1] == float(n), gate_ref[n:n + 1, :], 0.0)
    gate_row[...] = gate

    def at_rows(i):
        return pl.ds(pl.multiple_of((i // col_parts) * prow, prow), prow)

    def at_cols(i, base=0):
        return pl.ds(pl.multiple_of(base + (i % col_parts) * pcol, LANES), pcol)

    def project(i, owner):
        return jnp.dot(
            attended[at_rows(i), :], w_ref[:, at_cols(i, owner * out_width)],
            preferred_element_type=f32,
        )

    def pair_copy(i):
        return remote(pair_send.at[i], pair_recv.at[i], pair_ss.at[i], pair_rs.at[i], head=pair)

    def near_copy(i):
        return remote(near_send.at[i], near_recv.at[i], near_ss.at[i], near_rs.at[i], head=pair)

    def far_copy(i):
        return remote(far_send.at[i], far_recv.at[i], far_ss.at[i], far_rs.at[i], head=far)

    def slide_copy(i):
        return remote(
            upd_stage.at[i], next_hbm.at[at_rows(i), at_cols(i)], slide_ss.at[i], slide_rs.at[i],
            frame=f - 1,
        )

    def vel_copy(i):
        return pltpu.make_async_copy(
            vel_stage.at[i], vel_hbm.at[at_rows(i), at_cols(i)], vel_sem.at[i]
        )

    diagonal = (pair + 2) % 4

    def send_pair(i):
        pair_send[i] = project(i, diagonal).astype(bf16)
        pair_copy(i).start()

    def merge_head(h, carry):
        for t in range(tiles):
            merge(h, t)
        return carry

    lax.fori_loop(0, heads - 1, merge_head, 0)
    merge(heads - 1, 0)
    send_pair(0)

    def exchange(i, carry):
        for t in range(1, row_parts):
            @pl.when(i == t * col_parts - 2)
            def _():
                merge(heads - 1, t)

        @pl.when(i + 1 < pieces)
        def _():
            send_pair(i + 1)

        @pl.when(i < pieces)
        def _():
            mine = project(i, far)
            pair_copy(i).wait_recv()
            far_send[i] = (mine.astype(bf16).astype(f32) + pair_recv[i].astype(f32)).astype(bf16)
            far_copy(i).start()
            near_send[i] = project(i, pair).astype(bf16)
            near_copy(i).start()

        @pl.when(i >= lag)
        def _():
            join(i - lag)
        return carry

    def join(i):
        total = project(i, me).astype(bf16).astype(f32)
        near_copy(i).wait_recv()
        far_copy(i).wait_recv()
        total = total + near_recv[i].astype(f32) + far_recv[i].astype(f32)
        gated = gate_row[0:1, at_cols(i)] * total
        upd_stage[i] = (lat_ref[at_rows(i), at_cols(i)].astype(f32) + delta * gated).astype(bf16)

        @pl.when(has_prev)
        def _():
            slide_copy(i).start()
        vel_stage[i] = gated.astype(bf16)
        vel_copy(i).start()

    lax.fori_loop(0, pieces + lag, exchange, 0)

    for h in range(heads):
        @pl.when(even & has_next)
        def _():
            k_copy(h).wait_send()
            v_copy(h).wait_send()

        @pl.when(has_down)
        def _():
            q_copy(h).wait_send()

        @pl.when(has_up)
        def _():
            for t in range(tiles):
                o_copy(h, t).wait_send()
                st_copy(h, t).wait_send()

    @pl.when(odd & has_next)
    def _():
        for h in range(heads):
            relay_keys(h).wait_send()
            relay_values(h).wait_send()

    @pl.when((even & has_up) | (odd & has_down))
    def _():
        for h in range(heads):
            forward_keys(h).wait_send()

    @pl.when(has_down)
    def _():
        pen_copy.wait_send()

    @pl.when(f == frames - 1)
    def _():
        fresh_in = pltpu.make_async_copy(fresh_hbm, lat_ref, bulk_sem.at[0])
        fresh_in.start()
        fresh_in.wait()
        fresh_out = pltpu.make_async_copy(lat_ref, next_hbm, bulk_sem.at[1])
        fresh_out.start()
        fresh_out.wait()

    def drain(i, carry):
        pair_copy(i).wait_send()
        near_copy(i).wait_send()
        far_copy(i).wait_send()
        vel_copy(i).wait()

        @pl.when(has_prev)
        def _():
            slide_copy(i).wait_send()

        @pl.when(has_next)
        def _():
            slide_copy(i).wait_recv()
        return carry

    lax.fori_loop(0, pieces, drain, 0)


def shards(latents, queries, keys, values, out_weight, gate_table, levels, block_mask, fresh):
    span, hh = queries.shape
    heads = hh // HD
    out_width = latents.shape[1]
    assert lax.axis_size("head") == 4 and block_mask.shape[1] == 4
    assert out_weight.shape[1] == 4 * out_width and lax.axis_size("frame") % 2 == 0
    prow = span // 2
    pcol = 2 * LANES if out_width % (2 * LANES) == 0 else LANES
    pieces = (span // prow) * (out_width // pcol)

    vmem = pltpu.VMEM
    dma = pltpu.SemaphoreType.DMA
    tiles = span // prow
    head_block = vmem((heads, span, HD), bf16)
    head_wide = vmem((heads, span, HD), f32)
    stats = vmem((heads, tiles, 8, LANES), f32)
    piece = vmem((pieces, prow, pcol), bf16)
    any_spec = pl.BlockSpec(memory_space=pl.ANY)
    out = jax.ShapeDtypeStruct((span, out_width), bf16)
    return pl.pallas_call(
        kernel,
        in_specs=[any_spec] * 9,
        out_specs=[any_spec, any_spec],
        out_shape=[out, out],
        scratch_shapes=[pltpu.SMEM((1,), jnp.int32), pltpu.SMEM((1, 4), jnp.int32)]
        + [vmem(gate_table.shape, f32)]
        + [head_block] * 7
        + [vmem((8, LANES), f32)] * 2
        + [vmem((2 * span, 2 * HD), f32), vmem((2 * span, 1), f32), vmem((2 * span, span), bf16)]
        + [head_block, head_block, stats, stats, head_wide, head_wide]
        + [vmem((span, hh), bf16), vmem(out_weight.shape, bf16), vmem((span, out_width), bf16)]
        + [vmem((1, out_width), f32)]
        + [piece] * 8
        + [dma((heads, 3)), dma((5,)), dma((heads, 2)), dma((heads, 2))]
        + [dma((heads, 2))]
        + [dma((heads,))] * 4
        + [dma((heads, tiles))] * 4
        + [dma((2,))]
        + [dma((pieces,))] * 9,
        compiler_params=pltpu.CompilerParams(
            collective_id=0, has_side_effects=True, vmem_limit_bytes=VMEM_LIMIT
        ),
    )(
        levels, block_mask, queries, keys, values, out_weight, latents, fresh, gate_table
    )


def solution(mesh):
    in_specs = (
        P("frame", "head"),
        P("frame", "head"),
        P("frame", "head"),
        P("frame", "head"),
        P("head", None),
        P(None, "head"),
        P("frame"),
        P("frame", None),
        P(None, "head"),
    )
    out_specs = (P("frame", "head"), P("frame", "head"))
    return jax.shard_map(shards, mesh=mesh, in_specs=in_specs, out_specs=out_specs, check_vma=False)
```

```python
import functools
import math

import jax
import jax.numpy as jnp
from jax import lax
from jax.experimental import pallas as pl
from jax.experimental.pallas import tpu as pltpu
from jax.sharding import PartitionSpec as P

HD = 128
LANES = 128
LEVELS = 4
FAR = 1e30
LOW = -1e20
AHEAD = 3
LAG = 4
WIDE = 256
PIECE_ROWS = 256
PIECE_COLS = 128
VMEM_LIMIT = 60 * 1024 * 1024

flow_shift = 5.0

MESH = pl.DeviceIdType.MESH
bf16 = jnp.bfloat16
f32 = jnp.float32


def noise_level(point):
    return flow_shift * point / (1.0 + (flow_shift - 1.0) * point)


def scores_of(query, keys):
    scale = math.log2(math.e) / math.sqrt(HD)
    return lax.dot_general(query, keys, (((1,), (1,)), ((), ())), preferred_element_type=f32) * scale


def row_max(scores):
    top = jnp.max(scores, axis=1, keepdims=True)
    return jnp.broadcast_to(top, (scores.shape[0], LANES))


def across(stat, width):
    return jnp.concatenate([stat] * (width // LANES), axis=1)


def with_ones(values):
    return jnp.concatenate([values, jnp.ones((values.shape[0], LANES), bf16)], axis=1)


def kernel(
    levels_hbm, mask_hbm, q_hbm, k_hbm, v_hbm, w_hbm, lat_hbm, fresh_hbm, gate_hbm,
    vel_hbm, next_hbm,
    levels_ref, mask_ref, gate_ref,
    q_own, k_own, v_own, q_guest, k_prev, v_prev, relay, pen_own, pen_guest,
    acc_ref, top_ref, fade_ref, p_ref,
    o_send, o_recv, st_send, st_recv, o_loc, lse_loc, attended, w_ref, lat_ref, gate_row,
    pair_send, pair_recv, near_send, near_recv, far_send, far_recv, vel_stage, upd_stage,
    in_sem, bulk_sem, kv_ss, kv_rs, relay_ss, relay_rs, fwd_ss, q_ss, q_rs, o_ss, o_rs, st_ss, st_rs, pen_sem,
    pair_ss, pair_rs, near_ss, near_rs, far_ss, far_rs, vel_sem, slide_ss, slide_rs,
):
    f = lax.axis_index("frame")
    frames = lax.axis_size("frame")
    me = lax.axis_index("head")
    heads, span, _ = q_own.shape
    pieces, prow, pcol = pair_send.shape
    row_parts = span // prow
    col_parts = pieces // row_parts
    out_width = lat_ref.shape[1]
    tile = o_send.shape[1] // o_rs.shape[1]
    tiles = span // tile
    lag = min(LAG, pieces)

    pair = me + 1 - 2 * (me % 2)
    far = (me + 2) % 4
    odd = f % 2 == 1
    even = f % 2 == 0
    has_prev = f >= 1
    has_down = f >= 2
    has_next = f + 1 < frames
    has_up = f + 2 < frames

    def remote(src, dst, ss, rs, frame=None, head=None):
        where = {"frame": frame} if head is None else {"head": head}
        return pltpu.make_async_remote_copy(
            src_ref=src, dst_ref=dst, send_sem=ss, recv_sem=rs, device_id=where, device_id_type=MESH
        )

    def arrived(whole, sem):
        pltpu.make_async_copy(whole, whole, sem).wait()

    def columns(h):
        return pl.ds(pl.multiple_of(h * HD, HD), HD)

    def local_in(h):
        return [
            pltpu.make_async_copy(src.at[:, columns(h)], dst.at[h], in_sem.at[i])
            for i, (src, dst) in enumerate(((k_hbm, k_own), (q_hbm, q_own), (v_hbm, v_own)))
        ]

    w_in = pltpu.make_async_copy(w_hbm, w_ref, bulk_sem.at[0])
    lat_in = pltpu.make_async_copy(lat_hbm, lat_ref, bulk_sem.at[1])
    mask_in = pltpu.make_async_copy(mask_hbm, mask_ref, bulk_sem.at[2])
    levels_in = pltpu.make_async_copy(levels_hbm, levels_ref, bulk_sem.at[3])
    gate_in = pltpu.make_async_copy(gate_hbm, gate_ref, bulk_sem.at[4])

    def k_copy(h):
        return remote(k_own.at[h], k_prev.at[h], kv_ss.at[0], kv_rs.at[h, 0], frame=f + 1)

    def v_copy(h):
        return remote(v_own.at[h], v_prev.at[h], kv_ss.at[1], kv_rs.at[h, 1], frame=f + 1)

    def relay_keys(h):
        return remote(
            k_own.at[h], relay.at[h], relay_ss.at[0], relay_rs.at[h], frame=f - 1
        )

    def relay_values(h):
        return remote(
            v_own.at[h], relay.at[h], relay_ss.at[1], relay_rs.at[h], frame=f + 2
        )

    def forward_keys(h):
        return remote(relay.at[h], k_prev.at[h], fwd_ss, kv_rs.at[h, 0], frame=f + 2)

    def forward_values(h):
        return remote(relay.at[h], v_prev.at[h], fwd_ss, kv_rs.at[h, 1], frame=f - 1)

    def q_copy(h):
        return remote(q_own.at[h], q_guest.at[h], q_ss, q_rs.at[h], frame=f - 2)

    def o_copy(h, t):
        rows = pl.ds(t * tile, tile)
        return remote(
            o_send.at[h, rows], o_recv.at[h, rows], o_ss, o_rs.at[h, t], frame=f + 2
        )

    def st_copy(h, t):
        return remote(st_send.at[h, t], st_recv.at[h, t], st_ss, st_rs.at[h, t], frame=f + 2)

    pen_copy = remote(pen_own, pen_guest, pen_sem.at[0], pen_sem.at[1], frame=f - 2)

    barrier = pltpu.get_barrier_semaphore()
    for there, step in ((has_prev, -1), (has_down, -2), (has_next, 1), (has_up, 2)):
        @pl.when(there)
        def _():
            pl.semaphore_signal(barrier, inc=1, device_id={"frame": f + step}, device_id_type=MESH)
    for peer in (pair, far):
        pl.semaphore_signal(barrier, inc=1, device_id={"head": peer}, device_id_type=MESH)

    mask_in.start()
    for h in range(heads):
        for copy in local_in(h):
            copy.start()

    @pl.when(f == 0)
    def _():
        k_prev[...] = jnp.zeros_like(k_prev)
        v_prev[...] = jnp.zeros_like(v_prev)

    @pl.when(f < 2)
    def _():
        o_recv[...] = jnp.zeros_like(o_recv)
        st_recv[...] = jnp.full(st_recv.shape, LOW, f32)

    @pl.when(f + 2 >= frames)
    def _():
        q_guest[...] = jnp.zeros_like(q_guest)
        pen_guest[...] = jnp.zeros_like(pen_guest)

    mask_in.wait()
    for k in range(4):
        allowed = (mask_ref[0, k] == 1) & (f - k >= 0)
        pen_own[k:k + 1, :] = jnp.full((1, LANES), jnp.where(allowed, 0.0, FAR), f32)
    pen_own[4:, :] = jnp.zeros((4, LANES), f32)

    others = (
        2 + has_prev.astype(jnp.int32) + has_down.astype(jnp.int32)
        + has_next.astype(jnp.int32) + has_up.astype(jnp.int32)
    )
    pl.semaphore_wait(barrier, others)
    for i, whole in enumerate((k_own, q_own, v_own)):
        arrived(whole, in_sem.at[i])

    @pl.when(even & has_next)
    def _():
        for h in range(heads):
            k_copy(h).start()
            v_copy(h).start()

    @pl.when(odd & has_next)
    def _():
        for h in range(heads):
            relay_values(h).start()
        for h in range(AHEAD):
            relay_keys(h).start()

    @pl.when(has_down)
    def _():
        pen_copy.start()
        for h in range(heads):
            q_copy(h).start()

    w_in.start()
    levels_in.start()
    gate_in.start()
    lat_in.start()

    eye = lax.broadcasted_iota(jnp.int32, (LANES, LANES), 0) == lax.broadcasted_iota(
        jnp.int32, (LANES, LANES), 1
    )

    def merge(h, t):
        @pl.when(has_down)
        def _():
            o_copy(h, t).wait_recv()
            st_copy(h, t).wait_recv()
        for a in range(tile // LANES):
            rows = pl.ds(t * tile + a * LANES, LANES)
            guest_lse = jnp.sum(
                jnp.where(eye, st_recv[h, t, a:a + 1, :], 0.0), axis=1, keepdims=True
            )
            share = 1.0 / (1.0 + jnp.exp2(lse_loc[h, rows, :] - guest_lse))
            mine = o_loc[h, rows, :]
            both = mine + share * (o_recv[h, rows, :].astype(f32) - mine)
            attended[rows, columns(h)] = both.astype(bf16)

    @pl.when(has_up)
    def _():
        pen_copy.wait_recv()

    def forward(h):
        @pl.when(even & has_up)
        def _():
            relay_keys(h).wait_recv()
            forward_keys(h).start()

        @pl.when(odd & has_down)
        def _():
            relay_values(h).wait_recv()
            forward_values(h).start()

        @pl.when(odd & has_next & (h + AHEAD < heads))
        def _():
            relay_keys(h + AHEAD).start()

    levels_in.wait()
    gate_in.wait()
    level = jnp.full((1, LANES), levels_ref[0], jnp.int32).astype(f32)
    delta = (noise_level(level / LEVELS) - noise_level((level + 1.0) / LEVELS))[:, 0:1]
    gate = jnp.zeros((1, out_width), f32)
    for n in range(LEVELS):
        gate = gate + jnp.where(level[:, 0:1] == float(n), gate_ref[n:n + 1, :], 0.0)
    gate_row[...] = gate

    forward(0)

    wide = min(WIDE, span)
    row_tiles = [(q_guest, pen_guest, 2, t, True) for t in range(span // wide)]
    row_tiles += [(q_own, pen_own, 0, t, False) for t in range(span // wide)]

    def own_part(h):
        @pl.when(has_up)
        def _():
            q_copy(h).wait_recv()

        own_wide = with_ones(v_own[h])
        for n, (q_ref, pen_ref, first, t, _) in enumerate(row_tiles):
            at = pl.ds(n * wide, wide)
            s = scores_of(q_ref[h, pl.ds(t * wide, wide), :], k_own[h])
            penalty = pen_ref[first:first + 1, :]
            top = jnp.maximum(row_max(s) - penalty, LOW)
            weights = jnp.exp2(s - across(top + penalty, span)).astype(bf16)
            acc_ref[h % 2, at, :] = jnp.dot(weights, own_wide, preferred_element_type=f32)
            top_ref[h % 2, at, :] = top

    own_part(0)
    forward(1)

    def one_head(h, carry):
        @pl.when(has_prev)
        def _():
            k_copy(h).wait_recv()

        for n, (q_ref, pen_ref, first, t, _) in enumerate(row_tiles):
            at = pl.ds(n * wide, wide)
            s = scores_of(q_ref[h, pl.ds(t * wide, wide), :], k_prev[h])
            penalty = pen_ref[first + 1:first + 2, :]
            before = top_ref[h % 2, at, :]
            top = jnp.maximum(row_max(s) - penalty, before)
            p_ref[at, :] = jnp.exp2(s - across(top + penalty, span)).astype(bf16)
            fade_ref[at, :] = jnp.exp2(before - top)
            top_ref[h % 2, at, :] = top

        @pl.when(h + 2 < heads)
        def _():
            forward(h + 2)

        @pl.when(h + 1 < heads)
        def _():
            own_part(h + 1)

        @pl.when(has_prev)
        def _():
            v_copy(h).wait_recv()

        prev_wide = with_ones(v_prev[h])
        for n in range(2 * tiles):
            guest, t = n < tiles, n % tiles
            at = pl.ds(n * tile, tile)
            acc = acc_ref[h % 2, at, :] * across(fade_ref[at, :], 2 * HD)
            acc = acc + jnp.dot(p_ref[at, :], prev_wide, preferred_element_type=f32)
            total = jnp.maximum(acc[:, HD:], 1.0)
            out = acc[:, :HD] / total
            lse = top_ref[h % 2, at, :] + jnp.log2(total)
            rows = pl.ds(t * tile, tile)
            if guest:
                o_send[h, rows, :] = out.astype(bf16)
                for a in range(tile // LANES):
                    st_send[h, t, a:a + 1, :] = jnp.sum(
                        jnp.where(eye, lse[a * LANES:(a + 1) * LANES, :], 0.0), axis=0, keepdims=True
                    )

                @pl.when(has_up)
                def _():
                    st_copy(h, t).start()
                    o_copy(h, t).start()
            else:
                o_loc[h, rows, :] = out
                lse_loc[h, rows, :] = lse

        @pl.when(h >= 2)
        def _():
            for t in range(tiles):
                merge(h - 2, t)
        return carry

    lax.fori_loop(0, heads, one_head, 0)

    w_in.wait()
    lat_in.wait()

    def at_rows(i):
        return pl.ds(pl.multiple_of((i // col_parts) * prow, prow), prow)

    def at_cols(i, base=0):
        return pl.ds(pl.multiple_of(base + (i % col_parts) * pcol, LANES), pcol)

    def project(i, owner):
        return jnp.dot(
            attended[at_rows(i), :], w_ref[:, at_cols(i, owner * out_width)],
            preferred_element_type=f32,
        )

    def pair_copy(i):
        return remote(pair_send.at[i], pair_recv.at[i], pair_ss, pair_rs.at[i], head=pair)

    def near_copy(i):
        return remote(near_send.at[i], near_recv.at[i], near_ss, near_rs.at[i], head=pair)

    def far_copy(i):
        return remote(far_send.at[i], far_recv.at[i], far_ss, far_rs.at[i], head=far)

    def slide_copy(i):
        return remote(
            upd_stage.at[i], next_hbm.at[at_rows(i), at_cols(i)], slide_ss, slide_rs,
            frame=f - 1,
        )

    def vel_copy(i):
        return pltpu.make_async_copy(
            vel_stage.at[i], vel_hbm.at[at_rows(i), at_cols(i)], vel_sem
        )

    diagonal = (pair + 2) % 4

    def send_pair(i):
        pair_send[i] = project(i, diagonal).astype(bf16)
        pair_copy(i).start()

    for t in range(tiles):
        merge(heads - 2, t)
    merge(heads - 1, 0)
    send_pair(0)

    def exchange(i, carry):
        for t in range(1, tiles):
            @pl.when(i == t * (pieces // tiles) - 2)
            def _():
                merge(heads - 1, t)

        @pl.when(i + 1 < pieces)
        def _():
            send_pair(i + 1)

        @pl.when(i < pieces)
        def _():
            mine = project(i, far)
            pair_copy(i).wait_recv()
            far_send[i] = (mine.astype(bf16).astype(f32) + pair_recv[i].astype(f32)).astype(bf16)
            far_copy(i).start()
            near_send[i] = project(i, pair).astype(bf16)
            near_copy(i).start()

        @pl.when(i >= lag)
        def _():
            join(i - lag)
        return carry

    def join(i):
        total = project(i, me).astype(bf16).astype(f32)
        near_copy(i).wait_recv()
        far_copy(i).wait_recv()
        total = total + near_recv[i].astype(f32) + far_recv[i].astype(f32)
        gated = gate_row[0:1, at_cols(i)] * total
        upd_stage[i] = (lat_ref[at_rows(i), at_cols(i)].astype(f32) + delta * gated).astype(bf16)

        @pl.when(has_prev)
        def _():
            slide_copy(i).start()
        vel_stage[i] = gated.astype(bf16)
        vel_copy(i).start()

    lax.fori_loop(0, pieces + lag, exchange, 0)

    @pl.when(even & has_next)
    def _():
        arrived(k_own, kv_ss.at[0])
        arrived(v_own, kv_ss.at[1])

    @pl.when(odd & has_next)
    def _():
        arrived(k_own, relay_ss.at[0])
        arrived(v_own, relay_ss.at[1])

    @pl.when((even & has_up) | (odd & has_down))
    def _():
        arrived(relay, fwd_ss)

    @pl.when(has_up)
    def _():
        arrived(o_send, o_ss)
        arrived(st_send, st_ss)

    @pl.when(has_down)
    def _():
        arrived(q_own, q_ss)

    @pl.when(has_down)
    def _():
        pen_copy.wait_send()

    @pl.when(f == frames - 1)
    def _():
        fresh_in = pltpu.make_async_copy(fresh_hbm, lat_ref, bulk_sem.at[0])
        fresh_in.start()
        fresh_in.wait()
        fresh_out = pltpu.make_async_copy(lat_ref, next_hbm, bulk_sem.at[1])
        fresh_out.start()
        fresh_out.wait()

    arrived(pair_send, pair_ss)
    arrived(near_send, near_ss)
    arrived(far_send, far_ss)
    arrived(vel_stage, vel_sem)

    @pl.when(has_prev)
    def _():
        arrived(upd_stage, slide_ss)

    @pl.when(has_next)
    def _():
        arrived(upd_stage, slide_rs)


def shards(latents, queries, keys, values, out_weight, gate_table, levels, block_mask, fresh):
    span, hh = queries.shape
    heads = hh // HD
    out_width = latents.shape[1]
    assert lax.axis_size("head") == 4 and block_mask.shape[1] == 4
    assert out_weight.shape[1] == 4 * out_width and lax.axis_size("frame") % 2 == 0
    tiles = 2
    prow, pcol = min(PIECE_ROWS, span // tiles), PIECE_COLS
    assert span % (tiles * prow) == 0 and out_width % pcol == 0
    pieces = (span // prow) * (out_width // pcol)

    vmem = pltpu.VMEM
    dma = pltpu.SemaphoreType.DMA
    head_block = vmem((heads, span, HD), bf16)
    head_wide = vmem((heads, span, HD), f32)
    stats = vmem((heads, tiles, 8, LANES), f32)
    piece = vmem((pieces, prow, pcol), bf16)
    any_spec = pl.BlockSpec(memory_space=pl.ANY)
    out = jax.ShapeDtypeStruct((span, out_width), bf16)
    return pl.pallas_call(
        kernel,
        in_specs=[any_spec] * 9,
        out_specs=[any_spec, any_spec],
        out_shape=[out, out],
        scratch_shapes=[pltpu.SMEM((1,), jnp.int32), pltpu.SMEM((1, 4), jnp.int32)]
        + [vmem(gate_table.shape, f32)]
        + [head_block] * 7
        + [vmem((8, LANES), f32)] * 2
        + [vmem((2, 2 * span, 2 * HD), f32), vmem((2, 2 * span, LANES), f32)]
        + [vmem((2 * span, LANES), f32), vmem((2 * span, span), bf16)]
        + [head_block, head_block, stats, stats, head_wide, head_wide]
        + [vmem((span, hh), bf16), vmem(out_weight.shape, bf16), vmem((span, out_width), bf16)]
        + [vmem((1, out_width), f32)]
        + [piece] * 8
        + [dma((3,)), dma((5,)), dma((2,)), dma((heads, 2)), dma((2,)), dma((heads,)), dma(())]
        + [dma(()), dma((heads,))]
        + [dma(()), dma((heads, tiles))] * 2
        + [dma((2,))]
        + [dma(()), dma((pieces,))] * 3
        + [dma(())] * 3,
        compiler_params=pltpu.CompilerParams(
            collective_id=0, has_side_effects=True, vmem_limit_bytes=VMEM_LIMIT
        ),
    )(
        levels, block_mask, queries, keys, values, out_weight, latents, fresh, gate_table
    )


def solution(mesh):
    in_specs = (
        P("frame", "head"),
        P("frame", "head"),
        P("frame", "head"),
        P("frame", "head"),
        P("head", None),
        P(None, "head"),
        P("frame"),
        P("frame", None),
        P(None, "head"),
    )
    out_specs = (P("frame", "head"), P("frame", "head"))
    return jax.shard_map(shards, mesh=mesh, in_specs=in_specs, out_specs=out_specs, check_vma=False)
```

```python
import functools
import math

import jax
import jax.numpy as jnp
from jax import lax
from jax.experimental import pallas as pl
from jax.experimental.pallas import tpu as pltpu
from jax.sharding import PartitionSpec as P

HD = 128
LANES = 128
LEVELS = 4
FAR = 1e30
LOW = -1e20
AHEAD = 3
LAG = 4
WIDE = 256
PIECE_ROWS = 256
PIECE_COLS = 128
VMEM_LIMIT = 60 * 1024 * 1024

flow_shift = 5.0

MESH = pl.DeviceIdType.MESH
bf16 = jnp.bfloat16
f32 = jnp.float32


def noise_level(point):
    return flow_shift * point / (1.0 + (flow_shift - 1.0) * point)


def scores_of(query, keys):
    scale = math.log2(math.e) / math.sqrt(HD)
    return lax.dot_general(query, keys, (((1,), (1,)), ((), ())), preferred_element_type=f32) * scale


def row_max(scores):
    top = jnp.max(scores, axis=1, keepdims=True)
    return jnp.broadcast_to(top, (scores.shape[0], LANES))


def across(stat, width):
    return jnp.concatenate([stat] * (width // LANES), axis=1)


def with_ones(values):
    return jnp.concatenate([values, jnp.ones((values.shape[0], LANES), bf16)], axis=1)


def kernel(
    levels_hbm, mask_hbm, q_hbm, k_hbm, v_hbm, w_hbm, lat_hbm, fresh_hbm, gate_hbm,
    vel_hbm, next_hbm,
    levels_ref, mask_ref, gate_ref,
    q_own, k_own, v_own, q_guest, k_prev, v_prev, relay, pen_own, pen_guest,
    acc_ref, top_ref, fade_ref, p_ref,
    o_send, o_recv, st_send, st_recv, o_loc, lse_loc, attended, w_ref, lat_ref, gate_row,
    pair_send, pair_recv, near_send, near_recv, far_send, far_recv, vel_stage, upd_stage,
    in_sem, bulk_sem, kv_ss, kv_rs, relay_ss, relay_rs, fwd_ss, q_ss, q_rs, o_ss, o_rs, st_ss, st_rs, pen_sem,
    pair_ss, pair_rs, near_ss, near_rs, far_ss, far_rs, vel_sem, slide_ss, slide_rs,
):
    f = lax.axis_index("frame")
    frames = lax.axis_size("frame")
    me = lax.axis_index("head")
    heads, span, _ = q_own.shape
    pieces, prow, pcol = pair_send.shape
    row_parts = span // prow
    col_parts = pieces // row_parts
    out_width = lat_ref.shape[1]
    tile = o_send.shape[1] // o_rs.shape[1]
    tiles = span // tile
    lag = min(LAG, pieces)

    pair = me + 1 - 2 * (me % 2)
    far = (me + 2) % 4
    odd = f % 2 == 1
    even = f % 2 == 0
    has_prev = f >= 1
    has_down = f >= 2
    has_next = f + 1 < frames
    has_up = f + 2 < frames

    def remote(src, dst, ss, rs, frame=None, head=None):
        where = {"frame": frame} if head is None else {"head": head}
        return pltpu.make_async_remote_copy(
            src_ref=src, dst_ref=dst, send_sem=ss, recv_sem=rs, device_id=where, device_id_type=MESH
        )

    def arrived(whole, sem):
        pltpu.make_async_copy(whole, whole, sem).wait()

    def columns(h):
        return pl.ds(pl.multiple_of(h * HD, HD), HD)

    def local_in(h):
        return [
            pltpu.make_async_copy(src.at[:, columns(h)], dst.at[h], in_sem.at[i])
            for i, (src, dst) in enumerate(((k_hbm, k_own), (q_hbm, q_own), (v_hbm, v_own)))
        ]

    w_in = pltpu.make_async_copy(w_hbm, w_ref, bulk_sem.at[0])
    lat_in = pltpu.make_async_copy(lat_hbm, lat_ref, bulk_sem.at[1])
    mask_in = pltpu.make_async_copy(mask_hbm, mask_ref, bulk_sem.at[2])
    levels_in = pltpu.make_async_copy(levels_hbm, levels_ref, bulk_sem.at[3])
    gate_in = pltpu.make_async_copy(gate_hbm, gate_ref, bulk_sem.at[4])

    def k_copy(h):
        return remote(k_own.at[h], k_prev.at[h], kv_ss.at[0], kv_rs.at[h, 0], frame=f + 1)

    def v_copy(h):
        return remote(v_own.at[h], v_prev.at[h], kv_ss.at[1], kv_rs.at[h, 1], frame=f + 1)

    def relay_keys(h):
        return remote(
            k_own.at[h], relay.at[h], relay_ss.at[0], relay_rs.at[h], frame=f - 1
        )

    def relay_values(h):
        return remote(
            v_own.at[h], relay.at[h], relay_ss.at[1], relay_rs.at[h], frame=f + 2
        )

    def forward_keys(h):
        return remote(relay.at[h], k_prev.at[h], fwd_ss, kv_rs.at[h, 0], frame=f + 2)

    def forward_values(h):
        return remote(relay.at[h], v_prev.at[h], fwd_ss, kv_rs.at[h, 1], frame=f - 1)

    def q_copy(h):
        return remote(q_own.at[h], q_guest.at[h], q_ss, q_rs.at[h], frame=f - 2)

    def o_copy(h, t):
        rows = pl.ds(t * tile, tile)
        return remote(
            o_send.at[h, rows], o_recv.at[h, rows], o_ss, o_rs.at[h, t], frame=f + 2
        )

    def st_copy(h, t):
        return remote(st_send.at[h, t], st_recv.at[h, t], st_ss, st_rs.at[h, t], frame=f + 2)

    pen_copy = remote(pen_own, pen_guest, pen_sem.at[0], pen_sem.at[1], frame=f - 2)

    barrier = pltpu.get_barrier_semaphore()
    for there, step in ((has_prev, -1), (has_down, -2), (has_next, 1), (has_up, 2)):
        @pl.when(there)
        def _():
            pl.semaphore_signal(barrier, inc=1, device_id={"frame": f + step}, device_id_type=MESH)
    for peer in (pair, far):
        pl.semaphore_signal(barrier, inc=1, device_id={"head": peer}, device_id_type=MESH)

    mask_in.start()
    for h in range(heads):
        for copy in local_in(h):
            copy.start()

    @pl.when(f == 0)
    def _():
        k_prev[...] = jnp.zeros_like(k_prev)
        v_prev[...] = jnp.zeros_like(v_prev)

    @pl.when(f < 2)
    def _():
        o_recv[...] = jnp.zeros_like(o_recv)
        st_recv[...] = jnp.full(st_recv.shape, LOW, f32)

    @pl.when(f + 2 >= frames)
    def _():
        q_guest[...] = jnp.zeros_like(q_guest)
        pen_guest[...] = jnp.zeros_like(pen_guest)

    mask_in.wait()
    for k in range(4):
        allowed = (mask_ref[0, k] == 1) & (f - k >= 0)
        pen_own[k:k + 1, :] = jnp.full((1, LANES), jnp.where(allowed, 0.0, FAR), f32)
    pen_own[4:, :] = jnp.zeros((4, LANES), f32)

    others = (
        2 + has_prev.astype(jnp.int32) + has_down.astype(jnp.int32)
        + has_next.astype(jnp.int32) + has_up.astype(jnp.int32)
    )
    pl.semaphore_wait(barrier, others)
    for i, whole in enumerate((k_own, q_own, v_own)):
        arrived(whole, in_sem.at[i])

    @pl.when(even & has_next)
    def _():
        for h in range(heads):
            k_copy(h).start()
            v_copy(h).start()

    @pl.when(odd & has_next)
    def _():
        for h in range(heads):
            if h < AHEAD:
                relay_keys(h).start()
            relay_values(h).start()

    @pl.when(has_down)
    def _():
        pen_copy.start()
        for h in range(heads):
            q_copy(h).start()

    w_in.start()
    levels_in.start()
    gate_in.start()
    lat_in.start()

    eye = lax.broadcasted_iota(jnp.int32, (LANES, LANES), 0) == lax.broadcasted_iota(
        jnp.int32, (LANES, LANES), 1
    )

    def merge(h, t):
        @pl.when(has_down)
        def _():
            o_copy(h, t).wait_recv()
            st_copy(h, t).wait_recv()
        for a in range(tile // LANES):
            rows = pl.ds(t * tile + a * LANES, LANES)
            guest_lse = jnp.sum(
                jnp.where(eye, st_recv[h, t, a:a + 1, :], 0.0), axis=1, keepdims=True
            )
            share = 1.0 / (1.0 + jnp.exp2(lse_loc[h, rows, :] - guest_lse))
            mine = o_loc[h, rows, :]
            both = mine + share * (o_recv[h, rows, :].astype(f32) - mine)
            attended[rows, columns(h)] = both.astype(bf16)

    @pl.when(has_up)
    def _():
        pen_copy.wait_recv()

    def forward(h):
        @pl.when(even & has_up)
        def _():
            relay_keys(h).wait_recv()
            forward_keys(h).start()

        @pl.when(odd & has_down)
        def _():
            relay_values(h).wait_recv()
            forward_values(h).start()

        @pl.when(odd & has_next & (h + AHEAD < heads))
        def _():
            relay_keys(h + AHEAD).start()

    levels_in.wait()
    gate_in.wait()
    level = jnp.full((1, LANES), levels_ref[0], jnp.int32).astype(f32)
    delta = (noise_level(level / LEVELS) - noise_level((level + 1.0) / LEVELS))[:, 0:1]
    gate = jnp.zeros((1, out_width), f32)
    for n in range(LEVELS):
        gate = gate + jnp.where(level[:, 0:1] == float(n), gate_ref[n:n + 1, :], 0.0)
    gate_row[...] = gate

    forward(0)

    wide = min(WIDE, span)
    row_tiles = [(q_guest, pen_guest, 2, t, True) for t in range(span // wide)]
    row_tiles += [(q_own, pen_own, 0, t, False) for t in range(span // wide)]

    def own_part(h):
        @pl.when(has_up)
        def _():
            q_copy(h).wait_recv()

        own_wide = with_ones(v_own[h])
        for n, (q_ref, pen_ref, first, t, _) in enumerate(row_tiles):
            at = pl.ds(n * wide, wide)
            s = scores_of(q_ref[h, pl.ds(t * wide, wide), :], k_own[h])
            penalty = pen_ref[first:first + 1, :]
            top = jnp.maximum(row_max(s) - penalty, LOW)
            weights = jnp.exp2(s - across(top + penalty, span)).astype(bf16)
            acc_ref[h % 2, at, :] = jnp.dot(weights, own_wide, preferred_element_type=f32)
            top_ref[h % 2, at, :] = top

    own_part(0)
    forward(1)

    def one_head(h, carry):
        @pl.when(has_prev)
        def _():
            k_copy(h).wait_recv()

        for n, (q_ref, pen_ref, first, t, _) in enumerate(row_tiles):
            at = pl.ds(n * wide, wide)
            s = scores_of(q_ref[h, pl.ds(t * wide, wide), :], k_prev[h])
            penalty = pen_ref[first + 1:first + 2, :]
            before = top_ref[h % 2, at, :]
            top = jnp.maximum(row_max(s) - penalty, before)
            p_ref[at, :] = jnp.exp2(s - across(top + penalty, span)).astype(bf16)
            fade_ref[at, :] = jnp.exp2(before - top)
            top_ref[h % 2, at, :] = top

        @pl.when(h + 2 < heads)
        def _():
            forward(h + 2)

        @pl.when(h + 1 < heads)
        def _():
            own_part(h + 1)

        @pl.when(has_prev)
        def _():
            v_copy(h).wait_recv()

        prev_wide = with_ones(v_prev[h])
        for n in range(2 * tiles):
            guest, t = n < tiles, n % tiles
            at = pl.ds(n * tile, tile)
            acc = acc_ref[h % 2, at, :] * across(fade_ref[at, :], 2 * HD)
            acc = acc + jnp.dot(p_ref[at, :], prev_wide, preferred_element_type=f32)
            total = jnp.maximum(acc[:, HD:], 1.0)
            out = acc[:, :HD] / total
            lse = top_ref[h % 2, at, :] + jnp.log2(total)
            rows = pl.ds(t * tile, tile)
            if guest:
                o_send[h, rows, :] = out.astype(bf16)
                for a in range(tile // LANES):
                    st_send[h, t, a:a + 1, :] = jnp.sum(
                        jnp.where(eye, lse[a * LANES:(a + 1) * LANES, :], 0.0), axis=0, keepdims=True
                    )

                @pl.when(has_up)
                def _():
                    st_copy(h, t).start()
                    o_copy(h, t).start()
            else:
                o_loc[h, rows, :] = out
                lse_loc[h, rows, :] = lse

        @pl.when(h >= 2)
        def _():
            for t in range(tiles):
                merge(h - 2, t)
        return carry

    lax.fori_loop(0, heads, one_head, 0)

    w_in.wait()
    lat_in.wait()

    def at_rows(i):
        return pl.ds(pl.multiple_of((i // col_parts) * prow, prow), prow)

    def at_cols(i, base=0):
        return pl.ds(pl.multiple_of(base + (i % col_parts) * pcol, LANES), pcol)

    def project(i, owner):
        return jnp.dot(
            attended[at_rows(i), :], w_ref[:, at_cols(i, owner * out_width)],
            preferred_element_type=f32,
        )

    def pair_copy(i):
        return remote(pair_send.at[i], pair_recv.at[i], pair_ss, pair_rs.at[i], head=pair)

    def near_copy(i):
        return remote(near_send.at[i], near_recv.at[i], near_ss, near_rs.at[i], head=pair)

    def far_copy(i):
        return remote(far_send.at[i], far_recv.at[i], far_ss, far_rs.at[i], head=far)

    def slide_copy(i):
        return remote(
            upd_stage.at[i], next_hbm.at[at_rows(i), at_cols(i)], slide_ss, slide_rs,
            frame=f - 1,
        )

    def vel_copy(i):
        return pltpu.make_async_copy(
            vel_stage.at[i], vel_hbm.at[at_rows(i), at_cols(i)], vel_sem
        )

    diagonal = (pair + 2) % 4

    def send_pair(i):
        pair_send[i] = project(i, diagonal).astype(bf16)
        pair_copy(i).start()

    for t in range(tiles):
        merge(heads - 2, t)
    merge(heads - 1, 0)
    send_pair(0)

    def exchange(i, carry):
        for t in range(1, tiles):
            @pl.when(i == t * (pieces // tiles) - 2)
            def _():
                merge(heads - 1, t)

        @pl.when(i + 1 < pieces)
        def _():
            send_pair(i + 1)

        @pl.when(i < pieces)
        def _():
            mine = project(i, far)
            pair_copy(i).wait_recv()
            far_send[i] = (mine.astype(bf16).astype(f32) + pair_recv[i].astype(f32)).astype(bf16)
            far_copy(i).start()
            near_send[i] = project(i, pair).astype(bf16)
            near_copy(i).start()

        @pl.when(i >= lag)
        def _():
            join(i - lag)
        return carry

    def join(i):
        total = project(i, me).astype(bf16).astype(f32)
        near_copy(i).wait_recv()
        far_copy(i).wait_recv()
        total = total + near_recv[i].astype(f32) + far_recv[i].astype(f32)
        gated = gate_row[0:1, at_cols(i)] * total
        upd_stage[i] = (lat_ref[at_rows(i), at_cols(i)].astype(f32) + delta * gated).astype(bf16)

        @pl.when(has_prev)
        def _():
            slide_copy(i).start()
        vel_stage[i] = gated.astype(bf16)
        vel_copy(i).start()

    lax.fori_loop(0, pieces + lag, exchange, 0)

    @pl.when(even & has_next)
    def _():
        arrived(k_own, kv_ss.at[0])
        arrived(v_own, kv_ss.at[1])

    @pl.when(odd & has_next)
    def _():
        arrived(k_own, relay_ss.at[0])
        arrived(v_own, relay_ss.at[1])

    @pl.when((even & has_up) | (odd & has_down))
    def _():
        arrived(relay, fwd_ss)

    @pl.when(has_up)
    def _():
        arrived(o_send, o_ss)
        arrived(st_send, st_ss)

    @pl.when(has_down)
    def _():
        arrived(q_own, q_ss)

    @pl.when(has_down)
    def _():
        pen_copy.wait_send()

    @pl.when(f == frames - 1)
    def _():
        fresh_in = pltpu.make_async_copy(fresh_hbm, lat_ref, bulk_sem.at[0])
        fresh_in.start()
        fresh_in.wait()
        fresh_out = pltpu.make_async_copy(lat_ref, next_hbm, bulk_sem.at[1])
        fresh_out.start()
        fresh_out.wait()

    arrived(pair_send, pair_ss)
    arrived(near_send, near_ss)
    arrived(far_send, far_ss)
    arrived(vel_stage, vel_sem)

    @pl.when(has_prev)
    def _():
        arrived(upd_stage, slide_ss)

    @pl.when(has_next)
    def _():
        arrived(upd_stage, slide_rs)


def settle_kernel(a_hbm, b_hbm, a_out, b_out, stage, in_sem, out_sem):
    count, rows, _ = stage.shape
    half = count // 2
    ins, outs = [], []
    for i in range(count):
        src, dst = (a_hbm, a_out) if i < half else (b_hbm, b_out)
        at = pl.ds((i % half) * rows, rows)
        ins.append(pltpu.make_async_copy(src.at[at], stage.at[i], in_sem.at[i]))
        outs.append(pltpu.make_async_copy(stage.at[i], dst.at[at], out_sem.at[i]))
        ins[-1].start()
    for copy_in, copy_out in zip(ins, outs):
        copy_in.wait()
        copy_out.start()
    for copy_out in outs:
        copy_out.wait()


def settle(a, b):
    count = 8
    rows, width = a.shape
    any_spec = pl.BlockSpec(memory_space=pl.ANY)
    out = jax.ShapeDtypeStruct(a.shape, a.dtype)
    return pl.pallas_call(
        settle_kernel,
        in_specs=[any_spec] * 2,
        out_specs=[any_spec] * 2,
        out_shape=[out, out],
        scratch_shapes=[
            pltpu.VMEM((count, 2 * rows // count, width), a.dtype),
            pltpu.SemaphoreType.DMA((count,)),
            pltpu.SemaphoreType.DMA((count,)),
        ],
        compiler_params=pltpu.CompilerParams(vmem_limit_bytes=VMEM_LIMIT),
    )(a, b)


def shards(latents, queries, keys, values, out_weight, gate_table, levels, block_mask, fresh):
    span, hh = queries.shape
    heads = hh // HD
    out_width = latents.shape[1]
    assert lax.axis_size("head") == 4 and block_mask.shape[1] == 4
    assert out_weight.shape[1] == 4 * out_width and lax.axis_size("frame") % 2 == 0
    tiles = 2
    prow, pcol = min(PIECE_ROWS, span // tiles), PIECE_COLS
    assert span % (tiles * prow) == 0 and out_width % pcol == 0
    pieces = (span // prow) * (out_width // pcol)

    vmem = pltpu.VMEM
    dma = pltpu.SemaphoreType.DMA
    head_block = vmem((heads, span, HD), bf16)
    head_wide = vmem((heads, span, HD), f32)
    stats = vmem((heads, tiles, 8, LANES), f32)
    piece = vmem((pieces, prow, pcol), bf16)
    any_spec = pl.BlockSpec(memory_space=pl.ANY)
    out = jax.ShapeDtypeStruct((span, out_width), bf16)
    velocity, next_latents = pl.pallas_call(
        kernel,
        in_specs=[any_spec] * 9,
        out_specs=[any_spec, any_spec],
        out_shape=[out, out],
        scratch_shapes=[pltpu.SMEM((1,), jnp.int32), pltpu.SMEM((1, 4), jnp.int32)]
        + [vmem(gate_table.shape, f32)]
        + [head_block] * 7
        + [vmem((8, LANES), f32)] * 2
        + [vmem((2, 2 * span, 2 * HD), f32), vmem((2, 2 * span, LANES), f32)]
        + [vmem((2 * span, LANES), f32), vmem((2 * span, span), bf16)]
        + [head_block, head_block, stats, stats, head_wide, head_wide]
        + [vmem((span, hh), bf16), vmem(out_weight.shape, bf16), vmem((span, out_width), bf16)]
        + [vmem((1, out_width), f32)]
        + [piece] * 8
        + [dma((3,)), dma((5,)), dma((2,)), dma((heads, 2)), dma((2,)), dma((heads,)), dma(())]
        + [dma(()), dma((heads,))]
        + [dma(()), dma((heads, tiles))] * 2
        + [dma((2,))]
        + [dma(()), dma((pieces,))] * 3
        + [dma(())] * 3,
        compiler_params=pltpu.CompilerParams(
            collective_id=0, has_side_effects=True, vmem_limit_bytes=VMEM_LIMIT
        ),
    )(
        levels, block_mask, queries, keys, values, out_weight, latents, fresh, gate_table
    )
    return settle(velocity, next_latents)


def solution(mesh):
    in_specs = (
        P("frame", "head"),
        P("frame", "head"),
        P("frame", "head"),
        P("frame", "head"),
        P("head", None),
        P(None, "head"),
        P("frame"),
        P("frame", None),
        P(None, "head"),
    )
    out_specs = (P("frame", "head"), P("frame", "head"))
    return jax.shard_map(shards, mesh=mesh, in_specs=in_specs, out_specs=out_specs, check_vma=False)
```

```python
import functools
import math

import jax
import jax.numpy as jnp
from jax import lax
from jax.experimental import pallas as pl
from jax.experimental.pallas import tpu as pltpu
from jax.sharding import PartitionSpec as P

HD = 128
LANES = 128
LEVELS = 4
FAR = 1e30
LOW = -1e20
AHEAD = 3
LAG = 4
WIDE = 256
PIECE_ROWS = 256
PIECE_COLS = 128
VMEM_LIMIT = 60 * 1024 * 1024

flow_shift = 5.0

MESH = pl.DeviceIdType.MESH
bf16 = jnp.bfloat16
f32 = jnp.float32


def noise_level(point):
    return flow_shift * point / (1.0 + (flow_shift - 1.0) * point)


def scores_of(query, keys):
    scale = math.log2(math.e) / math.sqrt(HD)
    return lax.dot_general(query, keys, (((1,), (1,)), ((), ())), preferred_element_type=f32) * scale


def row_max(scores):
    top = jnp.max(scores, axis=1, keepdims=True)
    return jnp.broadcast_to(top, (scores.shape[0], LANES))


def across(stat, width):
    return jnp.concatenate([stat] * (width // LANES), axis=1)


def with_ones(values):
    return jnp.concatenate([values, jnp.ones((values.shape[0], LANES), bf16)], axis=1)


def kernel(
    levels_hbm, mask_hbm, q_hbm, k_hbm, v_hbm, w_hbm, lat_hbm, fresh_hbm, gate_hbm,
    vel_hbm, next_hbm,
    levels_ref, mask_ref, gate_ref,
    q_own, k_own, v_own, q_guest, k_prev, v_prev, relay, pen_own, pen_guest,
    acc_ref, top_ref, fade_ref, p_ref,
    o_send, o_recv, st_send, st_recv, o_loc, lse_loc, attended, w_ref, lat_ref, gate_row,
    pair_send, pair_recv, near_send, near_recv, far_send, far_recv, vel_stage, upd_stage,
    in_sem, bulk_sem, kv_ss, kv_rs, relay_ss, relay_rs, fwd_ss, q_ss, q_rs, o_ss, o_rs, st_ss, st_rs, pen_sem,
    pair_ss, pair_rs, near_ss, near_rs, far_ss, far_rs, vel_sem, slide_ss, slide_rs,
):
    f = lax.axis_index("frame")
    frames = lax.axis_size("frame")
    me = lax.axis_index("head")
    heads, span, _ = q_own.shape
    pieces, prow, pcol = pair_send.shape
    row_parts = span // prow
    col_parts = pieces // row_parts
    out_width = lat_ref.shape[1]
    tile = o_send.shape[1] // o_rs.shape[1]
    tiles = span // tile
    lag = min(LAG, pieces)

    pair = me + 1 - 2 * (me % 2)
    far = (me + 2) % 4
    odd = f % 2 == 1
    even = f % 2 == 0
    has_prev = f >= 1
    has_down = f >= 2
    has_next = f + 1 < frames
    has_up = f + 2 < frames

    def remote(src, dst, ss, rs, frame=None, head=None):
        where = {"frame": frame} if head is None else {"head": head}
        return pltpu.make_async_remote_copy(
            src_ref=src, dst_ref=dst, send_sem=ss, recv_sem=rs, device_id=where, device_id_type=MESH
        )

    def arrived(whole, sem):
        pltpu.make_async_copy(whole, whole, sem).wait()

    def columns(h):
        return pl.ds(pl.multiple_of(h * HD, HD), HD)

    def local_in(h):
        return [
            pltpu.make_async_copy(src.at[:, columns(h)], dst.at[h], in_sem.at[i])
            for i, (src, dst) in enumerate(((k_hbm, k_own), (q_hbm, q_own), (v_hbm, v_own)))
        ]

    w_in = pltpu.make_async_copy(w_hbm, w_ref, bulk_sem.at[0])
    lat_in = pltpu.make_async_copy(lat_hbm, lat_ref, bulk_sem.at[1])
    mask_in = pltpu.make_async_copy(mask_hbm, mask_ref, bulk_sem.at[2])
    levels_in = pltpu.make_async_copy(levels_hbm, levels_ref, bulk_sem.at[3])
    gate_in = pltpu.make_async_copy(gate_hbm, gate_ref, bulk_sem.at[4])

    def k_copy(h):
        return remote(k_own.at[h], k_prev.at[h], kv_ss.at[0], kv_rs.at[h, 0], frame=f + 1)

    def v_copy(h):
        return remote(v_own.at[h], v_prev.at[h], kv_ss.at[1], kv_rs.at[h, 1], frame=f + 1)

    def relay_keys(h):
        return remote(
            k_own.at[h], relay.at[h], relay_ss.at[0], relay_rs.at[h], frame=f - 1
        )

    def relay_values(h):
        return remote(
            v_own.at[h], relay.at[h], relay_ss.at[1], relay_rs.at[h], frame=f + 2
        )

    def forward_keys(h):
        return remote(relay.at[h], k_prev.at[h], fwd_ss, kv_rs.at[h, 0], frame=f + 2)

    def forward_values(h):
        return remote(relay.at[h], v_prev.at[h], fwd_ss, kv_rs.at[h, 1], frame=f - 1)

    def q_copy(h):
        return remote(q_own.at[h], q_guest.at[h], q_ss, q_rs.at[h], frame=f - 2)

    def o_copy(h, t):
        rows = pl.ds(t * tile, tile)
        return remote(
            o_send.at[h, rows], o_recv.at[h, rows], o_ss, o_rs.at[h, t], frame=f + 2
        )

    def st_copy(h, t):
        return remote(st_send.at[h, t], st_recv.at[h, t], st_ss, st_rs.at[h, t], frame=f + 2)

    pen_copy = remote(pen_own, pen_guest, pen_sem.at[0], pen_sem.at[1], frame=f - 2)

    barrier = pltpu.get_barrier_semaphore()
    for there, step in ((has_prev, -1), (has_down, -2), (has_next, 1), (has_up, 2)):
        @pl.when(there)
        def _():
            pl.semaphore_signal(barrier, inc=1, device_id={"frame": f + step}, device_id_type=MESH)
    for peer in (pair, far):
        pl.semaphore_signal(barrier, inc=1, device_id={"head": peer}, device_id_type=MESH)

    mask_in.start()
    for h in range(heads):
        for copy in local_in(h):
            copy.start()

    @pl.when(f == 0)
    def _():
        k_prev[...] = jnp.zeros_like(k_prev)
        v_prev[...] = jnp.zeros_like(v_prev)

    @pl.when(f < 2)
    def _():
        o_recv[...] = jnp.zeros_like(o_recv)
        st_recv[...] = jnp.full(st_recv.shape, LOW, f32)

    @pl.when(f + 2 >= frames)
    def _():
        q_guest[...] = jnp.zeros_like(q_guest)
        pen_guest[...] = jnp.zeros_like(pen_guest)

    mask_in.wait()
    for k in range(4):
        allowed = (mask_ref[0, k] == 1) & (f - k >= 0)
        pen_own[k:k + 1, :] = jnp.full((1, LANES), jnp.where(allowed, 0.0, FAR), f32)
    pen_own[4:, :] = jnp.zeros((4, LANES), f32)

    others = (
        2 + has_prev.astype(jnp.int32) + has_down.astype(jnp.int32)
        + has_next.astype(jnp.int32) + has_up.astype(jnp.int32)
    )
    pl.semaphore_wait(barrier, others)
    for i, whole in enumerate((k_own, q_own, v_own)):
        arrived(whole, in_sem.at[i])

    @pl.when(even & has_next)
    def _():
        for h in range(heads):
            k_copy(h).start()
            v_copy(h).start()

    @pl.when(odd & has_next)
    def _():
        for h in range(heads):
            if h < AHEAD:
                relay_keys(h).start()
            relay_values(h).start()

    @pl.when(has_down)
    def _():
        pen_copy.start()
        for h in range(heads):
            q_copy(h).start()

    w_in.start()
    levels_in.start()
    gate_in.start()
    lat_in.start()

    eye = lax.broadcasted_iota(jnp.int32, (LANES, LANES), 0) == lax.broadcasted_iota(
        jnp.int32, (LANES, LANES), 1
    )

    def merge(h, t):
        @pl.when(has_down)
        def _():
            o_copy(h, t).wait_recv()
            st_copy(h, t).wait_recv()
        for a in range(tile // LANES):
            rows = pl.ds(t * tile + a * LANES, LANES)
            guest_lse = jnp.sum(
                jnp.where(eye, st_recv[h, t, a:a + 1, :], 0.0), axis=1, keepdims=True
            )
            share = 1.0 / (1.0 + jnp.exp2(lse_loc[h, rows, :] - guest_lse))
            mine = o_loc[h, rows, :]
            both = mine + share * (o_recv[h, rows, :].astype(f32) - mine)
            attended[rows, columns(h)] = both.astype(bf16)

    @pl.when(has_up)
    def _():
        pen_copy.wait_recv()

    def forward(h):
        @pl.when(even & has_up)
        def _():
            relay_keys(h).wait_recv()
            forward_keys(h).start()

        @pl.when(odd & has_down)
        def _():
            relay_values(h).wait_recv()
            forward_values(h).start()

        @pl.when(odd & has_next & (h + AHEAD < heads))
        def _():
            relay_keys(h + AHEAD).start()

    levels_in.wait()
    gate_in.wait()
    level = jnp.full((1, LANES), levels_ref[0], jnp.int32).astype(f32)
    delta = (noise_level(level / LEVELS) - noise_level((level + 1.0) / LEVELS))[:, 0:1]
    gate = jnp.zeros((1, out_width), f32)
    for n in range(LEVELS):
        gate = gate + jnp.where(level[:, 0:1] == float(n), gate_ref[n:n + 1, :], 0.0)
    gate_row[...] = gate

    forward(0)

    wide = min(WIDE, span)
    row_tiles = [(q_guest, pen_guest, 2, t, True) for t in range(span // wide)]
    row_tiles += [(q_own, pen_own, 0, t, False) for t in range(span // wide)]

    def own_part(h):
        @pl.when(has_up)
        def _():
            q_copy(h).wait_recv()

        own_wide = with_ones(v_own[h])
        for n, (q_ref, pen_ref, first, t, _) in enumerate(row_tiles):
            at = pl.ds(n * wide, wide)
            s = scores_of(q_ref[h, pl.ds(t * wide, wide), :], k_own[h])
            penalty = pen_ref[first:first + 1, :]
            top = jnp.maximum(row_max(s) - penalty, LOW)
            weights = jnp.exp2(s - across(top + penalty, span)).astype(bf16)
            acc_ref[h % 2, at, :] = jnp.dot(weights, own_wide, preferred_element_type=f32)
            top_ref[h % 2, at, :] = top

    own_part(0)
    forward(1)

    def one_head(h, carry):
        @pl.when(has_prev)
        def _():
            k_copy(h).wait_recv()

        for n, (q_ref, pen_ref, first, t, _) in enumerate(row_tiles):
            at = pl.ds(n * wide, wide)
            s = scores_of(q_ref[h, pl.ds(t * wide, wide), :], k_prev[h])
            penalty = pen_ref[first + 1:first + 2, :]
            before = top_ref[h % 2, at, :]
            top = jnp.maximum(row_max(s) - penalty, before)
            p_ref[at, :] = jnp.exp2(s - across(top + penalty, span)).astype(bf16)
            fade_ref[at, :] = jnp.exp2(before - top)
            top_ref[h % 2, at, :] = top

        @pl.when(h + 2 < heads)
        def _():
            forward(h + 2)

        @pl.when(h + 1 < heads)
        def _():
            own_part(h + 1)

        @pl.when(has_prev)
        def _():
            v_copy(h).wait_recv()

        prev_wide = with_ones(v_prev[h])
        for n in range(2 * tiles):
            guest, t = n < tiles, n % tiles
            at = pl.ds(n * tile, tile)
            acc = acc_ref[h % 2, at, :] * across(fade_ref[at, :], 2 * HD)
            acc = acc + jnp.dot(p_ref[at, :], prev_wide, preferred_element_type=f32)
            total = jnp.maximum(acc[:, HD:], 1.0)
            out = acc[:, :HD] / total
            lse = top_ref[h % 2, at, :] + jnp.log2(total)
            rows = pl.ds(t * tile, tile)
            if guest:
                o_send[h, rows, :] = out.astype(bf16)
                for a in range(tile // LANES):
                    st_send[h, t, a:a + 1, :] = jnp.sum(
                        jnp.where(eye, lse[a * LANES:(a + 1) * LANES, :], 0.0), axis=0, keepdims=True
                    )

                if t == 0:
                    @pl.when(has_up)
                    def _():
                        st_copy(h, 0).start()
                        o_copy(h, 0).start()
                else:
                    @pl.when(has_up & (h < heads - 2))
                    def _():
                        st_copy(h, t).start()
                        o_copy(h, t).start()

                    @pl.when(has_up & (h == heads - 1))
                    def _():
                        for late in range(max(heads - 2, 0), heads):
                            st_copy(late, t).start()
                            o_copy(late, t).start()
            else:
                o_loc[h, rows, :] = out
                lse_loc[h, rows, :] = lse

        @pl.when(h >= 2)
        def _():
            for t in range(tiles):
                merge(h - 2, t)
        return carry

    lax.fori_loop(0, heads, one_head, 0)

    w_in.wait()
    lat_in.wait()

    def at_rows(i):
        return pl.ds(pl.multiple_of((i // col_parts) * prow, prow), prow)

    def at_cols(i, base=0):
        return pl.ds(pl.multiple_of(base + (i % col_parts) * pcol, LANES), pcol)

    def project(i, owner):
        return jnp.dot(
            attended[at_rows(i), :], w_ref[:, at_cols(i, owner * out_width)],
            preferred_element_type=f32,
        )

    def pair_copy(i):
        return remote(pair_send.at[i], pair_recv.at[i], pair_ss, pair_rs.at[i], head=pair)

    def near_copy(i):
        return remote(near_send.at[i], near_recv.at[i], near_ss, near_rs.at[i], head=pair)

    def far_copy(i):
        return remote(far_send.at[i], far_recv.at[i], far_ss, far_rs.at[i], head=far)

    def slide_copy(i):
        return remote(
            upd_stage.at[i], next_hbm.at[at_rows(i), at_cols(i)], slide_ss, slide_rs,
            frame=f - 1,
        )

    def vel_copy(i):
        return pltpu.make_async_copy(
            vel_stage.at[i], vel_hbm.at[at_rows(i), at_cols(i)], vel_sem
        )

    diagonal = (pair + 2) % 4

    def send_pair(i):
        pair_send[i] = project(i, diagonal).astype(bf16)
        pair_copy(i).start()

    for h in range(max(heads - 2, 0), heads):
        merge(h, 0)
    send_pair(0)

    def exchange(i, carry):
        for t in range(1, tiles):
            @pl.when(i == t * (pieces // tiles) - 2)
            def _():
                for h in range(max(heads - 2, 0), heads):
                    merge(h, t)

        @pl.when(i + 1 < pieces)
        def _():
            send_pair(i + 1)

        @pl.when(i < pieces)
        def _():
            mine = project(i, far)
            pair_copy(i).wait_recv()
            far_send[i] = (mine.astype(bf16).astype(f32) + pair_recv[i].astype(f32)).astype(bf16)
            far_copy(i).start()
            near_send[i] = project(i, pair).astype(bf16)
            near_copy(i).start()

        @pl.when(i >= lag)
        def _():
            join(i - lag)
        return carry

    def join(i):
        total = project(i, me).astype(bf16).astype(f32)
        near_copy(i).wait_recv()
        far_copy(i).wait_recv()
        total = total + near_recv[i].astype(f32) + far_recv[i].astype(f32)
        gated = gate_row[0:1, at_cols(i)] * total
        upd_stage[i] = (lat_ref[at_rows(i), at_cols(i)].astype(f32) + delta * gated).astype(bf16)

        @pl.when(has_prev)
        def _():
            slide_copy(i).start()
        vel_stage[i] = gated.astype(bf16)
        vel_copy(i).start()

    lax.fori_loop(0, pieces + lag, exchange, 0)

    @pl.when(even & has_next)
    def _():
        arrived(k_own, kv_ss.at[0])
        arrived(v_own, kv_ss.at[1])

    @pl.when(odd & has_next)
    def _():
        arrived(k_own, relay_ss.at[0])
        arrived(v_own, relay_ss.at[1])

    @pl.when((even & has_up) | (odd & has_down))
    def _():
        arrived(relay, fwd_ss)

    @pl.when(has_up)
    def _():
        arrived(o_send, o_ss)
        arrived(st_send, st_ss)

    @pl.when(has_down)
    def _():
        arrived(q_own, q_ss)

    @pl.when(has_down)
    def _():
        pen_copy.wait_send()

    @pl.when(f == frames - 1)
    def _():
        fresh_in = pltpu.make_async_copy(fresh_hbm, lat_ref, bulk_sem.at[0])
        fresh_in.start()
        fresh_in.wait()
        fresh_out = pltpu.make_async_copy(lat_ref, next_hbm, bulk_sem.at[1])
        fresh_out.start()
        fresh_out.wait()

    arrived(pair_send, pair_ss)
    arrived(near_send, near_ss)
    arrived(far_send, far_ss)
    arrived(vel_stage, vel_sem)

    @pl.when(has_prev)
    def _():
        arrived(upd_stage, slide_ss)

    @pl.when(has_next)
    def _():
        arrived(upd_stage, slide_rs)


def settle_kernel(a_hbm, b_hbm, a_out, b_out, stage, in_sem, out_sem):
    count, rows, _ = stage.shape
    half = count // 2
    ins, outs = [], []
    for i in range(count):
        src, dst = (a_hbm, a_out) if i < half else (b_hbm, b_out)
        at = pl.ds((i % half) * rows, rows)
        ins.append(pltpu.make_async_copy(src.at[at], stage.at[i], in_sem.at[i]))
        outs.append(pltpu.make_async_copy(stage.at[i], dst.at[at], out_sem.at[i]))
        ins[-1].start()
    for copy_in, copy_out in zip(ins, outs):
        copy_in.wait()
        copy_out.start()
    for copy_out in outs:
        copy_out.wait()


def settle(a, b):
    count = 8
    rows, width = a.shape
    any_spec = pl.BlockSpec(memory_space=pl.ANY)
    out = jax.ShapeDtypeStruct(a.shape, a.dtype)
    return pl.pallas_call(
        settle_kernel,
        in_specs=[any_spec] * 2,
        out_specs=[any_spec] * 2,
        out_shape=[out, out],
        scratch_shapes=[
            pltpu.VMEM((count, 2 * rows // count, width), a.dtype),
            pltpu.SemaphoreType.DMA((count,)),
            pltpu.SemaphoreType.DMA((count,)),
        ],
        compiler_params=pltpu.CompilerParams(vmem_limit_bytes=VMEM_LIMIT),
    )(a, b)


def shards(latents, queries, keys, values, out_weight, gate_table, levels, block_mask, fresh):
    span, hh = queries.shape
    heads = hh // HD
    out_width = latents.shape[1]
    assert lax.axis_size("head") == 4 and block_mask.shape[1] == 4
    assert out_weight.shape[1] == 4 * out_width and lax.axis_size("frame") % 2 == 0
    tiles = 2
    prow, pcol = min(PIECE_ROWS, span // tiles), PIECE_COLS
    assert span % (tiles * prow) == 0 and out_width % pcol == 0
    pieces = (span // prow) * (out_width // pcol)

    vmem = pltpu.VMEM
    dma = pltpu.SemaphoreType.DMA
    head_block = vmem((heads, span, HD), bf16)
    head_wide = vmem((heads, span, HD), f32)
    stats = vmem((heads, tiles, 8, LANES), f32)
    piece = vmem((pieces, prow, pcol), bf16)
    any_spec = pl.BlockSpec(memory_space=pl.ANY)
    out = jax.ShapeDtypeStruct((span, out_width), bf16)
    velocity, next_latents = pl.pallas_call(
        kernel,
        in_specs=[any_spec] * 9,
        out_specs=[any_spec, any_spec],
        out_shape=[out, out],
        scratch_shapes=[pltpu.SMEM((1,), jnp.int32), pltpu.SMEM((1, 4), jnp.int32)]
        + [vmem(gate_table.shape, f32)]
        + [head_block] * 7
        + [vmem((8, LANES), f32)] * 2
        + [vmem((2, 2 * span, 2 * HD), f32), vmem((2, 2 * span, LANES), f32)]
        + [vmem((2 * span, LANES), f32), vmem((2 * span, span), bf16)]
        + [head_block, head_block, stats, stats, head_wide, head_wide]
        + [vmem((span, hh), bf16), vmem(out_weight.shape, bf16), vmem((span, out_width), bf16)]
        + [vmem((1, out_width), f32)]
        + [piece] * 8
        + [dma((3,)), dma((5,)), dma((2,)), dma((heads, 2)), dma((2,)), dma((heads,)), dma(())]
        + [dma(()), dma((heads,))]
        + [dma(()), dma((heads, tiles))] * 2
        + [dma((2,))]
        + [dma(()), dma((pieces,))] * 3
        + [dma(())] * 3,
        compiler_params=pltpu.CompilerParams(
            collective_id=0, has_side_effects=True, vmem_limit_bytes=VMEM_LIMIT
        ),
    )(
        levels, block_mask, queries, keys, values, out_weight, latents, fresh, gate_table
    )
    return settle(velocity, next_latents)


def solution(mesh):
    in_specs = (
        P("frame", "head"),
        P("frame", "head"),
        P("frame", "head"),
        P("frame", "head"),
        P("head", None),
        P(None, "head"),
        P("frame"),
        P("frame", None),
        P(None, "head"),
    )
    out_specs = (P("frame", "head"), P("frame", "head"))
    return jax.shard_map(shards, mesh=mesh, in_specs=in_specs, out_specs=out_specs, check_vma=False)
```

```python
import functools
import math

import jax
import jax.numpy as jnp
from jax import lax
from jax.experimental import pallas as pl
from jax.experimental.pallas import tpu as pltpu
from jax.sharding import PartitionSpec as P

HD = 128
LANES = 128
LEVELS = 4
FAR = 1e30
LOW = -1e20
AHEAD = 3
LAG = 4
WIDE = 256
PIECE_ROWS = 256
PIECE_COLS = 128
VMEM_LIMIT = 60 * 1024 * 1024

flow_shift = 5.0

MESH = pl.DeviceIdType.MESH
bf16 = jnp.bfloat16
f32 = jnp.float32


def noise_level(point):
    return flow_shift * point / (1.0 + (flow_shift - 1.0) * point)


def scores_of(query, keys):
    scale = math.log2(math.e) / math.sqrt(HD)
    return lax.dot_general(query, keys, (((1,), (1,)), ((), ())), preferred_element_type=f32) * scale


def row_max(scores):
    top = jnp.max(scores, axis=1, keepdims=True)
    return jnp.broadcast_to(top, (scores.shape[0], LANES))


def across(stat, width):
    return jnp.concatenate([stat] * (width // LANES), axis=1)


def with_ones(values):
    return jnp.concatenate([values, jnp.ones((values.shape[0], LANES), bf16)], axis=1)


def kernel(
    levels_hbm, mask_hbm, q_hbm, k_hbm, v_hbm, w_hbm, lat_hbm, fresh_hbm, gate_hbm,
    vel_hbm, next_hbm,
    levels_ref, mask_ref, gate_ref,
    q_own, k_own, v_own, q_guest, k_prev, v_prev, relay, pen_own, pen_guest,
    acc_ref, top_ref, fade_ref, p_ref,
    o_send, o_recv, st_send, st_recv, o_loc, lse_loc, attended, w_ref, lat_ref, gate_row,
    pair_send, pair_recv, near_send, near_recv, far_send, far_recv, vel_stage, upd_stage,
    in_sem, bulk_sem, kv_ss, kv_rs, relay_ss, relay_rs, fwd_ss, q_ss, q_rs, o_ss, o_rs, st_ss, st_rs, pen_sem,
    pair_ss, pair_rs, near_ss, near_rs, far_ss, far_rs, vel_sem, slide_ss, slide_rs,
):
    f = lax.axis_index("frame")
    frames = lax.axis_size("frame")
    me = lax.axis_index("head")
    heads, span, _ = q_own.shape
    pieces, prow, pcol = pair_send.shape
    row_parts = span // prow
    col_parts = pieces // row_parts
    out_width = lat_ref.shape[1]
    tile = o_send.shape[1] // o_rs.shape[1]
    tiles = span // tile
    lag = min(LAG, pieces)

    pair = me + 1 - 2 * (me % 2)
    far = (me + 2) % 4
    odd = f % 2 == 1
    even = f % 2 == 0
    has_prev = f >= 1
    has_down = f >= 2
    has_next = f + 1 < frames
    has_up = f + 2 < frames

    def remote(src, dst, ss, rs, frame=None, head=None):
        where = {"frame": frame} if head is None else {"head": head}
        return pltpu.make_async_remote_copy(
            src_ref=src, dst_ref=dst, send_sem=ss, recv_sem=rs, device_id=where, device_id_type=MESH
        )

    def arrived(whole, sem):
        pltpu.make_async_copy(whole, whole, sem).wait()

    def columns(h):
        return pl.ds(pl.multiple_of(h * HD, HD), HD)

    def local_in(h):
        return [
            pltpu.make_async_copy(src.at[:, columns(h)], dst.at[h], in_sem.at[i])
            for i, (src, dst) in enumerate(((k_hbm, k_own), (q_hbm, q_own), (v_hbm, v_own)))
        ]

    w_in = pltpu.make_async_copy(w_hbm, w_ref, bulk_sem.at[0])
    lat_in = pltpu.make_async_copy(lat_hbm, lat_ref, bulk_sem.at[1])
    mask_in = pltpu.make_async_copy(mask_hbm, mask_ref, bulk_sem.at[2])
    levels_in = pltpu.make_async_copy(levels_hbm, levels_ref, bulk_sem.at[3])
    gate_in = pltpu.make_async_copy(gate_hbm, gate_ref, bulk_sem.at[4])

    def k_copy(h):
        return remote(k_hbm.at[:, columns(h)], k_prev.at[h], kv_ss.at[0], kv_rs.at[h, 0], frame=f + 1)

    def v_copy(h):
        return remote(v_hbm.at[:, columns(h)], v_prev.at[h], kv_ss.at[1], kv_rs.at[h, 1], frame=f + 1)

    def relay_keys(h):
        return remote(
            k_hbm.at[:, columns(h)], relay.at[h], relay_ss.at[0], relay_rs.at[h], frame=f - 1
        )

    def relay_values(h):
        return remote(
            v_hbm.at[:, columns(h)], relay.at[h], relay_ss.at[1], relay_rs.at[h], frame=f + 2
        )

    def forward_keys(h):
        return remote(relay.at[h], k_prev.at[h], fwd_ss, kv_rs.at[h, 0], frame=f + 2)

    def forward_values(h):
        return remote(relay.at[h], v_prev.at[h], fwd_ss, kv_rs.at[h, 1], frame=f - 1)

    def q_copy(h):
        return remote(q_hbm.at[:, columns(h)], q_guest.at[h], q_ss, q_rs.at[h], frame=f - 2)

    def o_copy(h, t):
        rows = pl.ds(t * tile, tile)
        return remote(
            o_send.at[h, rows], o_recv.at[h, rows], o_ss, o_rs.at[h, t], frame=f + 2
        )

    def st_copy(h, t):
        return remote(st_send.at[h, t], st_recv.at[h, t], st_ss, st_rs.at[h, t], frame=f + 2)

    pen_copy = remote(pen_own, pen_guest, pen_sem.at[0], pen_sem.at[1], frame=f - 2)

    barrier = pltpu.get_barrier_semaphore()
    for there, step in ((has_prev, -1), (has_down, -2), (has_next, 1), (has_up, 2)):
        @pl.when(there)
        def _():
            pl.semaphore_signal(barrier, inc=1, device_id={"frame": f + step}, device_id_type=MESH)
    for peer in (pair, far):
        pl.semaphore_signal(barrier, inc=1, device_id={"head": peer}, device_id_type=MESH)

    mask_in.start()
    for h in range(heads):
        for copy in local_in(h):
            copy.start()

    @pl.when(f == 0)
    def _():
        k_prev[...] = jnp.zeros_like(k_prev)
        v_prev[...] = jnp.zeros_like(v_prev)

    @pl.when(f < 2)
    def _():
        o_recv[...] = jnp.zeros_like(o_recv)
        st_recv[...] = jnp.full(st_recv.shape, LOW, f32)

    @pl.when(f + 2 >= frames)
    def _():
        q_guest[...] = jnp.zeros_like(q_guest)
        pen_guest[...] = jnp.zeros_like(pen_guest)

    mask_in.wait()
    for k in range(4):
        allowed = (mask_ref[0, k] == 1) & (f - k >= 0)
        pen_own[k:k + 1, :] = jnp.full((1, LANES), jnp.where(allowed, 0.0, FAR), f32)
    pen_own[4:, :] = jnp.zeros((4, LANES), f32)

    others = (
        2 + has_prev.astype(jnp.int32) + has_down.astype(jnp.int32)
        + has_next.astype(jnp.int32) + has_up.astype(jnp.int32)
    )
    pl.semaphore_wait(barrier, others)
    @pl.when(even & has_next)
    def _():
        for h in range(heads):
            k_copy(h).start()
            v_copy(h).start()

    @pl.when(odd & has_next)
    def _():
        for h in range(heads):
            if h < AHEAD:
                relay_keys(h).start()
            relay_values(h).start()

    @pl.when(has_down)
    def _():
        pen_copy.start()
        for h in range(heads):
            q_copy(h).start()

    w_in.start()
    levels_in.start()
    gate_in.start()
    lat_in.start()

    eye = lax.broadcasted_iota(jnp.int32, (LANES, LANES), 0) == lax.broadcasted_iota(
        jnp.int32, (LANES, LANES), 1
    )

    def merge(h, t):
        @pl.when(has_down)
        def _():
            o_copy(h, t).wait_recv()
            st_copy(h, t).wait_recv()
        for a in range(tile // LANES):
            rows = pl.ds(t * tile + a * LANES, LANES)
            guest_lse = jnp.sum(
                jnp.where(eye, st_recv[h, t, a:a + 1, :], 0.0), axis=1, keepdims=True
            )
            share = 1.0 / (1.0 + jnp.exp2(lse_loc[h, rows, :] - guest_lse))
            mine = o_loc[h, rows, :]
            both = mine + share * (o_recv[h, rows, :].astype(f32) - mine)
            attended[rows, columns(h)] = both.astype(bf16)

    @pl.when(has_up)
    def _():
        pen_copy.wait_recv()

    def forward(h):
        @pl.when(even & has_up)
        def _():
            relay_keys(h).wait_recv()
            forward_keys(h).start()

        @pl.when(odd & has_down)
        def _():
            relay_values(h).wait_recv()
            forward_values(h).start()

        @pl.when(odd & has_next & (h + AHEAD < heads))
        def _():
            relay_keys(h + AHEAD).start()

    levels_in.wait()
    gate_in.wait()
    level = jnp.full((1, LANES), levels_ref[0], jnp.int32).astype(f32)
    delta = (noise_level(level / LEVELS) - noise_level((level + 1.0) / LEVELS))[:, 0:1]
    gate = jnp.zeros((1, out_width), f32)
    for n in range(LEVELS):
        gate = gate + jnp.where(level[:, 0:1] == float(n), gate_ref[n:n + 1, :], 0.0)
    gate_row[...] = gate

    forward(0)

    wide = min(WIDE, span)
    row_tiles = [(q_guest, pen_guest, 2, t, True) for t in range(span // wide)]
    row_tiles += [(q_own, pen_own, 0, t, False) for t in range(span // wide)]

    def own_part(h):
        @pl.when(has_up)
        def _():
            q_copy(h).wait_recv()

        own_wide = with_ones(v_own[h])
        for n, (q_ref, pen_ref, first, t, _) in enumerate(row_tiles):
            at = pl.ds(n * wide, wide)
            s = scores_of(q_ref[h, pl.ds(t * wide, wide), :], k_own[h])
            penalty = pen_ref[first:first + 1, :]
            top = jnp.maximum(row_max(s) - penalty, LOW)
            weights = jnp.exp2(s - across(top + penalty, span)).astype(bf16)
            acc_ref[h % 2, at, :] = jnp.dot(weights, own_wide, preferred_element_type=f32)
            top_ref[h % 2, at, :] = top

    for i, whole in enumerate((k_own, q_own, v_own)):
        arrived(whole, in_sem.at[i])

    own_part(0)
    forward(1)

    def one_head(h, carry):
        @pl.when(has_prev)
        def _():
            k_copy(h).wait_recv()

        for n, (q_ref, pen_ref, first, t, _) in enumerate(row_tiles):
            at = pl.ds(n * wide, wide)
            s = scores_of(q_ref[h, pl.ds(t * wide, wide), :], k_prev[h])
            penalty = pen_ref[first + 1:first + 2, :]
            before = top_ref[h % 2, at, :]
            top = jnp.maximum(row_max(s) - penalty, before)
            p_ref[at, :] = jnp.exp2(s - across(top + penalty, span)).astype(bf16)
            fade_ref[at, :] = jnp.exp2(before - top)
            top_ref[h % 2, at, :] = top

        @pl.when(h + 2 < heads)
        def _():
            forward(h + 2)

        @pl.when(h + 1 < heads)
        def _():
            own_part(h + 1)

        @pl.when(has_prev)
        def _():
            v_copy(h).wait_recv()

        prev_wide = with_ones(v_prev[h])
        for n in range(2 * tiles):
            guest, t = n < tiles, n % tiles
            at = pl.ds(n * tile, tile)
            acc = acc_ref[h % 2, at, :] * across(fade_ref[at, :], 2 * HD)
            acc = acc + jnp.dot(p_ref[at, :], prev_wide, preferred_element_type=f32)
            total = jnp.maximum(acc[:, HD:], 1.0)
            out = acc[:, :HD] / total
            lse = top_ref[h % 2, at, :] + jnp.log2(total)
            rows = pl.ds(t * tile, tile)
            if guest:
                o_send[h, rows, :] = out.astype(bf16)
                for a in range(tile // LANES):
                    st_send[h, t, a:a + 1, :] = jnp.sum(
                        jnp.where(eye, lse[a * LANES:(a + 1) * LANES, :], 0.0), axis=0, keepdims=True
                    )

                if t == 0:
                    @pl.when(has_up)
                    def _():
                        st_copy(h, 0).start()
                        o_copy(h, 0).start()
                else:
                    @pl.when(has_up & (h < heads - 2))
                    def _():
                        st_copy(h, t).start()
                        o_copy(h, t).start()

                    @pl.when(has_up & (h == heads - 1))
                    def _():
                        for late in range(max(heads - 2, 0), heads):
                            st_copy(late, t).start()
                            o_copy(late, t).start()
            else:
                o_loc[h, rows, :] = out
                lse_loc[h, rows, :] = lse

        @pl.when(h >= 2)
        def _():
            for t in range(tiles):
                merge(h - 2, t)
        return carry

    lax.fori_loop(0, heads, one_head, 0)

    w_in.wait()
    lat_in.wait()

    def at_rows(i):
        return pl.ds(pl.multiple_of((i // col_parts) * prow, prow), prow)

    def at_cols(i, base=0):
        return pl.ds(pl.multiple_of(base + (i % col_parts) * pcol, LANES), pcol)

    def project(i, owner):
        return jnp.dot(
            attended[at_rows(i), :], w_ref[:, at_cols(i, owner * out_width)],
            preferred_element_type=f32,
        )

    def pair_copy(i):
        return remote(pair_send.at[i], pair_recv.at[i], pair_ss, pair_rs.at[i], head=pair)

    def near_copy(i):
        return remote(near_send.at[i], near_recv.at[i], near_ss, near_rs.at[i], head=pair)

    def far_copy(i):
        return remote(far_send.at[i], far_recv.at[i], far_ss, far_rs.at[i], head=far)

    def slide_copy(i):
        return remote(
            upd_stage.at[i], next_hbm.at[at_rows(i), at_cols(i)], slide_ss, slide_rs,
            frame=f - 1,
        )

    def vel_copy(i):
        return pltpu.make_async_copy(
            vel_stage.at[i], vel_hbm.at[at_rows(i), at_cols(i)], vel_sem
        )

    diagonal = (pair + 2) % 4

    def send_pair(i):
        pair_send[i] = project(i, diagonal).astype(bf16)
        pair_copy(i).start()

    for h in range(max(heads - 2, 0), heads):
        merge(h, 0)
    send_pair(0)

    def exchange(i, carry):
        for t in range(1, tiles):
            @pl.when(i == t * (pieces // tiles) - 2)
            def _():
                for h in range(max(heads - 2, 0), heads):
                    merge(h, t)

        @pl.when(i + 1 < pieces)
        def _():
            send_pair(i + 1)

        @pl.when(i < pieces)
        def _():
            mine = project(i, far)
            pair_copy(i).wait_recv()
            far_send[i] = (mine.astype(bf16).astype(f32) + pair_recv[i].astype(f32)).astype(bf16)
            far_copy(i).start()
            near_send[i] = project(i, pair).astype(bf16)
            near_copy(i).start()

        @pl.when(i >= lag)
        def _():
            join(i - lag)
        return carry

    def join(i):
        total = project(i, me).astype(bf16).astype(f32)
        near_copy(i).wait_recv()
        far_copy(i).wait_recv()
        total = total + near_recv[i].astype(f32) + far_recv[i].astype(f32)
        gated = gate_row[0:1, at_cols(i)] * total
        upd_stage[i] = (lat_ref[at_rows(i), at_cols(i)].astype(f32) + delta * gated).astype(bf16)

        @pl.when(has_prev)
        def _():
            slide_copy(i).start()
        vel_stage[i] = gated.astype(bf16)
        vel_copy(i).start()

    lax.fori_loop(0, pieces + lag, exchange, 0)

    @pl.when(even & has_next)
    def _():
        arrived(k_own, kv_ss.at[0])
        arrived(v_own, kv_ss.at[1])

    @pl.when(odd & has_next)
    def _():
        arrived(k_own, relay_ss.at[0])
        arrived(v_own, relay_ss.at[1])

    @pl.when((even & has_up) | (odd & has_down))
    def _():
        arrived(relay, fwd_ss)

    @pl.when(has_up)
    def _():
        arrived(o_send, o_ss)
        arrived(st_send, st_ss)

    @pl.when(has_down)
    def _():
        arrived(q_own, q_ss)

    @pl.when(has_down)
    def _():
        pen_copy.wait_send()

    @pl.when(f == frames - 1)
    def _():
        fresh_in = pltpu.make_async_copy(fresh_hbm, lat_ref, bulk_sem.at[0])
        fresh_in.start()
        fresh_in.wait()
        fresh_out = pltpu.make_async_copy(lat_ref, next_hbm, bulk_sem.at[1])
        fresh_out.start()
        fresh_out.wait()

    arrived(pair_send, pair_ss)
    arrived(near_send, near_ss)
    arrived(far_send, far_ss)
    arrived(vel_stage, vel_sem)

    @pl.when(has_prev)
    def _():
        arrived(upd_stage, slide_ss)

    @pl.when(has_next)
    def _():
        arrived(upd_stage, slide_rs)


def settle_kernel(a_hbm, b_hbm, a_out, b_out, stage, in_sem, out_sem):
    count, rows, _ = stage.shape
    half = count // 2
    ins, outs = [], []
    for i in range(count):
        src, dst = (a_hbm, a_out) if i < half else (b_hbm, b_out)
        at = pl.ds((i % half) * rows, rows)
        ins.append(pltpu.make_async_copy(src.at[at], stage.at[i], in_sem.at[i]))
        outs.append(pltpu.make_async_copy(stage.at[i], dst.at[at], out_sem.at[i]))
        ins[-1].start()
    for copy_in, copy_out in zip(ins, outs):
        copy_in.wait()
        copy_out.start()
    for copy_out in outs:
        copy_out.wait()


def settle(a, b):
    count = 8
    rows, width = a.shape
    any_spec = pl.BlockSpec(memory_space=pl.ANY)
    out = jax.ShapeDtypeStruct(a.shape, a.dtype)
    return pl.pallas_call(
        settle_kernel,
        in_specs=[any_spec] * 2,
        out_specs=[any_spec] * 2,
        out_shape=[out, out],
        scratch_shapes=[
            pltpu.VMEM((count, 2 * rows // count, width), a.dtype),
            pltpu.SemaphoreType.DMA((count,)),
            pltpu.SemaphoreType.DMA((count,)),
        ],
        compiler_params=pltpu.CompilerParams(vmem_limit_bytes=VMEM_LIMIT),
    )(a, b)


def shards(latents, queries, keys, values, out_weight, gate_table, levels, block_mask, fresh):
    span, hh = queries.shape
    heads = hh // HD
    out_width = latents.shape[1]
    assert lax.axis_size("head") == 4 and block_mask.shape[1] == 4
    assert out_weight.shape[1] == 4 * out_width and lax.axis_size("frame") % 2 == 0
    tiles = 2
    prow, pcol = min(PIECE_ROWS, span // tiles), PIECE_COLS
    assert span % (tiles * prow) == 0 and out_width % pcol == 0
    pieces = (span // prow) * (out_width // pcol)

    vmem = pltpu.VMEM
    dma = pltpu.SemaphoreType.DMA
    head_block = vmem((heads, span, HD), bf16)
    head_wide = vmem((heads, span, HD), f32)
    stats = vmem((heads, tiles, 8, LANES), f32)
    piece = vmem((pieces, prow, pcol), bf16)
    any_spec = pl.BlockSpec(memory_space=pl.ANY)
    out = jax.ShapeDtypeStruct((span, out_width), bf16)
    velocity, next_latents = pl.pallas_call(
        kernel,
        in_specs=[any_spec] * 9,
        out_specs=[any_spec, any_spec],
        out_shape=[out, out],
        scratch_shapes=[pltpu.SMEM((1,), jnp.int32), pltpu.SMEM((1, 4), jnp.int32)]
        + [vmem(gate_table.shape, f32)]
        + [head_block] * 7
        + [vmem((8, LANES), f32)] * 2
        + [vmem((2, 2 * span, 2 * HD), f32), vmem((2, 2 * span, LANES), f32)]
        + [vmem((2 * span, LANES), f32), vmem((2 * span, span), bf16)]
        + [head_block, head_block, stats, stats, head_wide, head_wide]
        + [vmem((span, hh), bf16), vmem(out_weight.shape, bf16), vmem((span, out_width), bf16)]
        + [vmem((1, out_width), f32)]
        + [piece] * 8
        + [dma((3,)), dma((5,)), dma((2,)), dma((heads, 2)), dma((2,)), dma((heads,)), dma(())]
        + [dma(()), dma((heads,))]
        + [dma(()), dma((heads, tiles))] * 2
        + [dma((2,))]
        + [dma(()), dma((pieces,))] * 3
        + [dma(())] * 3,
        compiler_params=pltpu.CompilerParams(
            collective_id=0, has_side_effects=True, vmem_limit_bytes=VMEM_LIMIT
        ),
    )(
        levels, block_mask, queries, keys, values, out_weight, latents, fresh, gate_table
    )
    return settle(velocity, next_latents)


def solution(mesh):
    in_specs = (
        P("frame", "head"),
        P("frame", "head"),
        P("frame", "head"),
        P("frame", "head"),
        P("head", None),
        P(None, "head"),
        P("frame"),
        P("frame", None),
        P(None, "head"),
    )
    out_specs = (P("frame", "head"), P("frame", "head"))
    return jax.shard_map(shards, mesh=mesh, in_specs=in_specs, out_specs=out_specs, check_vma=False)
```
